512 devices in a mesh: groups: 2 (over y), row: 32 (over z), col: 4 (over x), chan: 2 (over core).
Axes of the slice: x: 4, y: 2, z: 32, core: 2. Of those that a mesh axis runs over, the one named last changes fastest.
The devices are a block of a 4x16x32 slice.
Arguments:
- pair_rep: bfloat16 [512, 256, 128], P(('groups', 'row'), 'col'), parts along dimension 0, may hold values from -6 to 6
- pair_mask: int32 [512, 256], P(('groups', 'row'), 'col'), parts along dimension 0, may hold values 0 or 1
- w_qkvg: bfloat16 [4, 128, 128], P(None, None, 'chan'), may hold values from -0.5 to 0.5
- w_bias: bfloat16 [128, 4], P(None, 'chan'), may hold values from -11 to 11
- w_out: bfloat16 [128, 128], P('chan'), may hold values from -0.5 to 0.5
- cotangent: bfloat16 [512, 256, 128], P(('groups', 'row'), 'col'), parts along dimension 0, may hold values from -6 to 6
Outputs:
- pair_update: bfloat16 [512, 256, 128], P(('groups', 'row'), 'col'), parts along dimension 0
- pair_grad: bfloat16 [512, 256, 128], P(('groups', 'row'), 'col'), parts along dimension 0
- qkvg_grad: float32 [8, 128, 128], P('groups', None, 'chan'), parts along dimension 0
- bias_weight_grad: float32 [256, 4], P('groups', 'chan'), parts along dimension 0
- out_weight_grad: float32 [128, 256], P('chan', 'groups'), parts along dimension 1
The draws below stay inside these ranges and needn't reach their ends.
There are 2 independent parts, one for each index of `groups`. The reference program is written for one: setup_inputs(seed, part) draws one part's arguments, and reference() takes and returns one part's arrays. A program takes and returns all parts, laid end to end along the dimension named above; an argument that names none is the same for every part. Nothing has to cross between parts.
All inputs are finite; a program needn't handle non-finite values. No bound on the sum of `pair_mask` on one device may be relied on, other than what follows from the above.
Results may differ from the reference program's by a relative error of at most 0.035.
The reference program's roundings to bfloat16 on the way count: a program that leaves them out, or rounds other values in their place, can miss the bound.
Values may be sent and summed in bfloat16 or wider, within the bound.
A program may use at most 64 MiB of HBM per device.

```python
import math
import jax
import jax.numpy as jnp
from jax import lax

D = 128
HEADS = 4
DH = 32
N = 256
N_COL = 4


def draw_w_bias(key, part):
    normal_vals = jnp.clip(jax.random.normal(key, (D, HEADS), jnp.float32), -4.0, 4.0)
    scaled = jnp.clip(normal_vals / math.sqrt(D), -11.0, 11.0)
    return scaled.astype(jnp.bfloat16)


def plant(drawn, key, least, high):
    spot = [jax.random.randint(jax.random.fold_in(key, axis), (), 0, length) for axis, length in enumerate(drawn.shape)]
    longest = drawn.shape.index(max(drawn.shape))
    neighbour = spot[:longest] + [(spot[longest] + 1) % drawn.shape[longest]] + spot[longest + 1:]
    return drawn.at[tuple(spot)].set(least).at[tuple(neighbour)].set(high)


def raised(result, key, source, target, parts, factor):
    owner, partner = [(jnp.arange(result.shape[axis_at]) // (result.shape[axis_at] // parts)).reshape([-1 if axis == axis_at else 1 for axis in range(result.ndim)]) for axis_at in (source, target)]
    chosen = jax.random.permutation(key, parts)[partner]
    strong = (owner == chosen) | (owner == (partner + parts // 2) % parts)
    return jnp.where(strong, factor * result, result)


def shard_levels(key, extent, shards, low, high):
    def one(dim, blocks):
        draws = jax.random.uniform(jax.random.fold_in(jax.random.fold_in(key, 6), dim), (blocks,), jnp.float32, low / len(shards), high / len(shards))
        return jnp.repeat(jnp.exp(draws), extent[dim] // blocks).reshape((-1,) + (1,) * (len(extent) - dim - 1))

    factor_of = one(*shards[0])
    for cut in shards[1:]:
        factor_of = factor_of * one(*cut)
    return factor_of


def bell_draw(own_key, extent, scale, most, shards=(), kind=jnp.bfloat16):
    loudness = shard_levels(own_key, extent, shards, -0.22, 0.18) if shards else 1.0
    result = jax.random.normal(own_key, extent, jnp.float32) * scale * loudness
    return jnp.minimum(jnp.maximum(result, -most), most).astype(kind)


def bell_draw_with(key, shape, scale, most, cuts, heavy, held_as=jnp.bfloat16):
    drawn = scale * jax.random.normal(key, shape, jnp.float32)
    if cuts:
        drawn = drawn * shard_levels(key, shape, cuts, -0.22, 0.18)
    return jnp.clip(raised(drawn, jax.random.fold_in(key, 3), *heavy), -most, most).astype(held_as)


def setup_inputs(seed: int = 0, part: int = 0) -> dict:
    key_of = jax.random.split(jax.random.key(seed), 7)
    part_keys = jax.random.split(jax.random.fold_in(key_of[6], part), 7)
    pair_rep = bell_draw(part_keys[0], (N, N, D), 1.0, 6.0, ((0, 32), (1, 4)))
    pair_mask = plant((jax.random.randint(part_keys[1], (N, N), 0, 8) < 7).astype(jnp.int32), jax.random.fold_in(part_keys[1], 1), 0, 1)
    w_qkvg = bell_draw(key_of[2], (4, D, HEADS * DH), D ** -0.5, 0.5, ((2, 2),))
    w_bias = draw_w_bias(jax.random.fold_in(key_of[6], 71), part)
    w_out = bell_draw(key_of[4], (HEADS * DH, D), (HEADS * DH) ** -0.5, 0.5, ((0, 2),))
    cotangent = bell_draw_with(part_keys[5], (N, N, D), 1.0, 6.0, ((0, 32), (1, 4)), (0, 1, 32, 2.75))
    return dict(pair_rep=pair_rep, pair_mask=pair_mask, w_qkvg=w_qkvg, w_bias=w_bias, w_out=w_out, cotangent=cotangent)


EPSILON = 1e-05
MASK_BIG = 1000000000.0
HIGH = lax.Precision.HIGHEST

def standardize(pair_rep):
    values = pair_rep.astype(jnp.float32)
    centred = values - lax.optimization_barrier(jnp.mean(values, -1, keepdims=True))
    inv_scale = lax.rsqrt(lax.optimization_barrier(jnp.mean(centred * centred, -1, keepdims=True)) + EPSILON)
    return (centred * inv_scale, inv_scale)

def rounded(values):
    return lax.optimization_barrier(values.astype(jnp.bfloat16)).astype(jnp.float32)

def reference(pair_rep, pair_mask, w_qkvg, w_bias, w_out, cotangent):
    standard, inv_scale = standardize(pair_rep)
    normed_wide = rounded(standard)
    weights_in = w_qkvg.astype(jnp.float32)
    bias_in = w_bias.astype(jnp.float32)
    out_in = w_out.astype(jnp.float32)
    pair_bias = jnp.einsum('jkc,ch->hjk', normed_wide, bias_in, precision=HIGH)
    query_scale = DH ** (-0.5)
    stride = 4
    block_cols = N // N_COL
    shaped = (stride, N, HEADS, DH)

    def split(values):
        return values.reshape((N // stride, stride) + values.shape[1:])

    def attend(running, inputs):
        bias_acc, qkvg_acc, out_acc = running
        normed_block, mask_block, cot_block = inputs
        cot_wide = cot_block.astype(jnp.float32)
        projected = jnp.einsum('bjc,pce->pbje', normed_block, weights_in, precision=HIGH)
        queries = rounded(projected[0] * query_scale).reshape(shaped)
        keys = rounded(projected[1]).reshape(shaped)
        values_b = rounded(projected[2]).reshape(shaped)
        gate_act = jax.nn.sigmoid(projected[3]).reshape(shaped)
        scores = jnp.einsum('bjhd,bkhd->bhjk', queries, keys, precision=HIGH)
        scores = scores + pair_bias[None] + MASK_BIG * (mask_block.astype(jnp.float32)[:, None, None, :] - 1.0)
        weights = jax.nn.softmax(scores, axis=-1)
        weights_b = rounded(weights)
        attended = jnp.einsum('bhjk,bkhd->bjhd', weights_b, values_b, precision=HIGH)
        gated = rounded(gate_act * attended).reshape(stride * N, HEADS * DH)
        update_rows = jnp.dot(gated, out_in, precision=HIGH).reshape(stride, N, D).astype(jnp.bfloat16)
        d_gated = jnp.dot(cot_wide.reshape(-1, D), out_in.T, precision=HIGH).reshape(shaped)
        d_gate = d_gated * attended * gate_act * (1.0 - gate_act)
        d_attended = rounded(d_gated * gate_act)
        d_weights = jnp.einsum('bjhd,bkhd->bhjk', d_attended, values_b, precision=HIGH)
        row_dot = lax.optimization_barrier(jnp.sum(d_attended * attended, -1)).transpose(0, 2, 1)[..., None]
        d_scores = weights * (d_weights - row_dot)
        d_scores_b = rounded(d_scores)
        d_query = jnp.einsum('bhjk,bkhd->bjhd', d_scores_b, keys, precision=HIGH) * query_scale
        blocked_scores = d_scores_b.reshape(stride, HEADS, N_COL, block_cols, N)
        blocked_weights = weights_b.reshape(stride, HEADS, N_COL, block_cols, N)
        blocked_query = queries.reshape(stride, N_COL, block_cols, HEADS, DH)
        blocked_attended = d_attended.reshape(stride, N_COL, block_cols, HEADS, DH)
        d_key = lax.optimization_barrier(jnp.sum(rounded(jnp.einsum('bhgjk,bgjhd->bgkhd', blocked_scores, blocked_query, precision=HIGH)), 1))
        d_value = lax.optimization_barrier(jnp.sum(rounded(jnp.einsum('bhgjk,bgjhd->bgkhd', blocked_weights, blocked_attended, precision=HIGH)), 1))
        d_proj = rounded(jnp.stack([d_query, d_key, d_value, d_gate]).reshape(4, stride, N, HEADS * DH))
        d_rows = jnp.einsum('pbje,pce->bjc', d_proj, weights_in, precision=HIGH)
        bias_acc = bias_acc + lax.optimization_barrier(jnp.sum(d_scores, 0))
        qkvg_acc = qkvg_acc + jnp.einsum('bjc,pbje->pce', normed_block, d_proj, precision=HIGH)
        out_acc = out_acc + jnp.dot(gated.T, cot_wide.reshape(-1, D), precision=HIGH)
        return ((bias_acc, qkvg_acc, out_acc), (update_rows, d_rows))
    start = (jnp.zeros((HEADS, N, N), jnp.float32), jnp.zeros((4, D, HEADS * DH), jnp.float32), jnp.zeros((HEADS * DH, D), jnp.float32))
    finals, stacked = lax.scan(attend, start, (split(normed_wide), split(pair_mask), split(cotangent)))
    bias_acc, qkvg_acc, out_acc = finals
    pair_update = stacked[0].reshape(N, N, D)
    d_normed = stacked[1].reshape(N, N, D) + jnp.einsum('hjk,ch->jkc', bias_acc, bias_in, precision=HIGH)
    centred_grad = d_normed - lax.optimization_barrier(jnp.mean(d_normed, -1, keepdims=True))
    centred_grad = centred_grad - standard * lax.optimization_barrier(jnp.mean(d_normed * standard, -1, keepdims=True))
    pair_grad = (inv_scale * centred_grad).astype(jnp.bfloat16)
    bias_weight_grad = jnp.einsum('jkc,hjk->ch', normed_wide, bias_acc, precision=HIGH) / N
    return (pair_update, pair_grad, qkvg_acc / N, bias_weight_grad, out_acc / N)
```

```python
import functools

import jax
import jax.numpy as jnp
from jax import lax
from jax.experimental import pallas as pl
from jax.experimental.pallas import tpu as pltpu
from jax.sharding import PartitionSpec as P

EPSILON = 1e-05
MASK_BIG = 1000000000.0
MESH = pl.DeviceIdType.MESH
F32 = jnp.float32
BF16 = jnp.bfloat16
HOP = 4
DMA = pltpu.SemaphoreType.DMA


def place(axis, step):
    size = lax.axis_size(axis)
    return lax.rem(lax.axis_index(axis) + (step % size), size)


def remote(src, dst, send, recv, axis, step):
    return pltpu.make_async_remote_copy(
        src_ref=src,
        dst_ref=dst,
        send_sem=send,
        recv_sem=recv,
        device_id={axis: place(axis, step)},
        device_id_type=MESH,
    )


def arrived(dst, recv):
    pltpu.make_async_copy(dst, dst, recv).wait()


def meet(chan):
    barrier = pltpu.get_barrier_semaphore()
    steps = [("row", s * t) for t in range(1, HOP + 1) for s in (1, -1)]
    steps += [("col", d) for d in range(1, lax.axis_size("col"))]
    if chan:
        steps += [("chan", 1)]
    for axis, step in steps:
        pl.semaphore_signal(
            barrier, inc=1, device_id={axis: place(axis, step)}, device_id_type=MESH
        )
    pl.semaphore_wait(barrier, len(steps))


def gather_everywhere(piece, out, zs, zr, xs, xr, beside):
    length, width = lax.axis_size("row"), lax.axis_size("col")
    x, half = lax.axis_index("col"), length // 2
    last = half // HOP

    def along_row(src, delta, steps):
        slot = out.at[x, place("row", -delta)]
        for step in steps:
            remote(src, slot, zs, zr.at[(delta + step) % length], "row", step).start()

    def along_col(src, delta):
        slot = out.at[x, place("row", -delta)]
        for d in range(1, width):
            remote(src, slot, xs, xr.at[d], "col", d).start()

    def slot_of(delta):
        return out.at[x, place("row", -delta)]

    along_row(piece, 0, [s * t for t in (HOP, 3, 2, 1) for s in (1, -1)])
    beside()
    along_col(piece, 0)
    out[x, lax.axis_index("row")] = piece[...]
    for a in range(1, last + 1):
        for s in (1, -1):
            if a == last:
                continue
            delta = s * HOP * a
            arrived(slot_of(delta), zr.at[delta % length])
            far = [s * HOP] if (s == 1 or a < last - 1) else []
            along_row(slot_of(delta), delta, far + [s * t for t in (3, 2, 1)])
        for s in (1, -1):
            if a < last:
                along_col(slot_of(s * HOP * a), s * HOP * a)
            for t in range(1, HOP):
                delta = s * (HOP * (a - 1) + t)
                arrived(slot_of(delta), zr.at[delta % length])
                along_col(slot_of(delta), delta)
    arrived(slot_of(half), zr.at[half])
    along_col(slot_of(half), half)
    for d in range(1, width):
        arrived(out.at[place("col", -d)], xr.at[d])
    rest = out.at[0, pl.ds(0, length - 1)]
    arrived(rest, zs)
    rest = out.at[pl.ds(0, width - 1)]
    arrived(rest, xs)


def exchange(src, dst, xs, xr):
    for d in range(1, lax.axis_size("col")):
        remote(
            src.at[place("col", d)], dst.at[lax.axis_index("col")], xs, xr.at[d], "col", d
        ).start()


def exchanged(dst, xs, xr):
    for d in range(1, lax.axis_size("col")):
        arrived(dst.at[place("col", -d)], xr.at[d])
    arrived(dst.at[pl.ds(0, lax.axis_size("col") - 1)], xs)


def gather_kernel(piece, tile, cot, mask, out, rows, cots, masks, zs, zr, xs, xr, es, er):
    meet(False)
    x = lax.axis_index("col")

    def beside():
        pairs = ((tile, rows), (cot, cots), (mask, masks))
        for n, (src, dst) in enumerate(pairs):
            exchange(src, dst, es.at[n], er.at[n])
        for src, dst in pairs:
            dst[x] = src[x]

    gather_everywhere(piece, out, zs, zr, xs, xr, beside)
    for n, dst in enumerate((rows, cots, masks)):
        exchanged(dst, es.at[n], er.at[n])


def over(a, b):
    return lax.dot_general(a, b, (((1,), (1,)), ((), ())), preferred_element_type=F32)


def under(a, b):
    return lax.dot_general(a, b, (((0,), (0,)), ((), ())), preferred_element_type=F32)


def plain(a, b):
    return lax.dot_general(a, b, (((1,), (0,)), ((), ())), preferred_element_type=F32)


def attend_kernel(
    scale, bias, rows, cots, masks, wqk, wvg, wout, d_bias, upd, dn, grads
):
    width, row_count, block, channels = rows.shape
    tokens = width * block
    cols = wout.shape[0]
    size = cols // 2
    head_lane = lax.broadcasted_iota(jnp.int32, (block, cols), 1) < size
    lane = lax.broadcasted_iota(jnp.int32, (tokens, 2 * block), 1) < block
    lane_col = lax.broadcasted_iota(jnp.int32, (tokens, cols), 1) < size
    span = 2 * block

    def doubled(values):
        parts = []
        for n in range(width):
            part = values[n * block : (n + 1) * block]
            zero = jnp.zeros_like(part)
            parts += [jnp.where(head_lane, part, zero), jnp.where(head_lane, zero, part)]
        return jnp.concatenate(parts, 0)

    def halved(values):
        parts = []
        for n in range(width):
            first = values[n * span : n * span + block]
            second = values[n * span + block : (n + 1) * span]
            parts += [jnp.where(head_lane, first, second)]
        return jnp.concatenate(parts, 0)

    def per_head(parts, joined, reduced, empty):
        both = functools.reduce(joined, parts)
        first = reduced(jnp.where(lane, both, empty), axis=1, keepdims=True)
        second = reduced(jnp.where(lane, empty, both), axis=1, keepdims=True)
        return jnp.where(lane, first, second)

    bias_sum = [None] * width
    gqk = gvg = gout = None
    for r in range(row_count):
        normed = rows[:, r].reshape(tokens, channels)
        cot = cots[:, r].reshape(tokens, channels)
        qk = plain(normed, wqk[...])
        vg = plain(normed, wvg[...])
        query = (qk[:, :cols] * scale).astype(BF16)
        key2 = doubled(qk[:, cols:]).astype(BF16)
        value2 = doubled(vg[:, :cols]).astype(BF16)
        gate = jax.nn.sigmoid(vg[:, cols:])
        scores = over(query, key2)
        parts = [
            (scores[:, n * span : (n + 1) * span] + bias[n]) + masks[n, r : r + 1, :]
            for n in range(width)
        ]
        top = per_head(parts, jnp.maximum, jnp.max, -jnp.inf)
        parts = [jnp.exp(part - top) for part in parts]
        inverse = 1.0 / per_head(parts, jnp.add, jnp.sum, 0.0)
        weights = [part * inverse for part in parts]
        weights_b = jnp.concatenate([w.astype(BF16) for w in weights], 1)
        attended = plain(weights_b, value2)
        gated = (gate * attended).astype(BF16)
        upd[:, r] = plain(gated, wout[...]).astype(BF16).reshape(width, block, channels)
        d_gated = over(cot, wout[...])
        d_gate = d_gated * attended * gate * (1.0 - gate)
        d_attended = (d_gated * gate).astype(BF16)
        d_weights = over(d_attended, value2)
        product = d_attended.astype(F32) * attended
        first = jnp.sum(jnp.where(lane_col, product, 0.0), axis=1, keepdims=True)
        second = jnp.sum(jnp.where(lane_col, 0.0, product), axis=1, keepdims=True)
        row_dot = jnp.where(lane, first, second)
        d_scores = [
            weights[n] * (d_weights[:, n * span : (n + 1) * span] - row_dot)
            for n in range(width)
        ]
        bias_sum = [d if b is None else b + d for b, d in zip(bias_sum, d_scores)]
        d_scores_b = jnp.concatenate([d.astype(BF16) for d in d_scores], 1)
        d_query = plain(d_scores_b, key2) * scale
        d_key = halved(under(d_scores_b, query))
        d_value = halved(under(weights_b, d_attended))
        dqk = jnp.concatenate([d_query, d_key], 1).astype(BF16)
        dvg = jnp.concatenate([d_value, d_gate], 1).astype(BF16)
        back = over(dqk, wqk[...]) + over(dvg, wvg[...])
        dn[:, r] = back.astype(BF16).reshape(width, block, channels)
        new = (under(normed, dqk), under(normed, dvg), under(gated, cot))
        if gqk is None:
            gqk, gvg, gout = new
        else:
            gqk, gvg, gout = gqk + new[0], gvg + new[1], gout + new[2]
    for n in range(width):
        d_bias[n] = bias_sum[n].astype(BF16)
    share = grads.shape[1]
    everything = jnp.concatenate([gqk, gvg, gout], 0).astype(BF16)
    for n in range(width):
        grads[n] = everything[n * share : (n + 1) * share]


def reduce_kernel(
    d_bias, grads, upd, dn, standard, inverse, w_bias, update, grad, final,
    bias_in, grads_in, upd_in, dn_in, upd_other, dn_mine, dn_other, pieces, plus, minus,
    acc_plus, acc_minus, send_plus, send_minus, piece, xs, xr, ls, lp, lm, ap, am, rs, cs, cr,
    gzs, gzr, gxs, gxr,
):
    length, width = lax.axis_size("row"), lax.axis_size("col")
    x, z = lax.axis_index("col"), lax.axis_index("row")
    half = length // 2
    chain = half // HOP
    row_count = d_bias.shape[1] // length
    meet(True)
    sources = ((d_bias, bias_in), (grads, grads_in), (upd, upd_in), (dn, dn_in))
    for n, (src, dst) in enumerate(sources):
        exchange(src, dst, xs.at[n], xr.at[n])
    for src, dst in sources:
        dst[x] = src[x]
    exchanged(bias_in, xs.at[0], xr.at[0])
    exchanged(grads_in, xs.at[1], xr.at[1])
    total = jnp.sum(bias_in[...].astype(F32), 0).reshape(length, row_count, -1)
    share = jnp.sum(grads_in[...].astype(F32), 0).reshape(-1, HOP, total.shape[-1])
    used = share.shape[0]
    share = jnp.concatenate(
        [share, jnp.zeros((length - used,) + share.shape[1:], F32)], 0
    )
    blank = jnp.zeros((length, pieces.shape[1] - row_count - HOP, total.shape[-1]), F32)
    pieces[...] = jnp.concatenate([total, share, blank], 1).astype(BF16)

    sides = ((1, plus, acc_plus, send_plus, lp, ap), (-1, minus, acc_minus, send_minus, lm, am))
    for a in range(chain - 1, -1, -1):
        for s, leaves, acc, _, leaf_sem, acc_sem in sides:
            if s == 1 and a == chain - 1:
                remote(
                    pieces.at[place("row", -half)], acc.at[a], ls, acc_sem.at[a], "row", -HOP
                ).start()
            for t in range(HOP - 1, 0, -1):
                remote(
                    pieces.at[place("row", -s * (t + HOP * a))],
                    leaves.at[a, t - 1],
                    ls,
                    leaf_sem.at[a],
                    "row",
                    -s * t,
                ).start()
    exchanged(upd_in, xs.at[2], xr.at[2])
    other = remote(upd_in, upd_other, cs.at[0], cr.at[0], "chan", 1)
    other.start()
    exchanged(dn_in, xs.at[3], xr.at[3])
    for a in range(chain - 1, 0, -1):
        for s, leaves, acc, out, leaf_sem, acc_sem in sides:
            arrived(leaves.at[a], leaf_sem.at[a])
            value = pieces[place("row", -s * HOP * a)].astype(F32)
            value = value + jnp.sum(leaves[a].astype(F32), 0)
            if s == 1 or a < chain - 1:
                arrived(acc.at[a], acc_sem.at[a])
                value = value + acc[a].astype(F32)
            out[a] = value.astype(BF16)
            remote(out.at[a], acc.at[a - 1], rs, acc_sem.at[a - 1], "row", -s * HOP).start()
        if a == chain - 1:
            other.wait()
            update[...] = (upd_in[...].astype(F32) + upd_other[...].astype(F32)).astype(BF16)
    value = pieces[z].astype(F32)
    for s, leaves, acc, out, leaf_sem, acc_sem in sides:
        arrived(leaves.at[0], leaf_sem.at[0])
        arrived(acc.at[0], acc_sem.at[0])
        value = value + jnp.sum(leaves[0].astype(F32), 0) + acc[0].astype(F32)
    tile = value[:row_count]
    columns = jnp.transpose(tile)
    block = columns.shape[0] // 2
    sums = [None, None]
    for j in range(row_count):
        normed = standard[j // 2, j % 2].astype(BF16).astype(F32)
        added = dn_in[j // 2, j % 2].astype(F32)
        for h in range(2):
            column = columns[h * block : (h + 1) * block, j : j + 1]
            added = added + column * w_bias[h : h + 1, :]
            term = normed * column
            sums[h] = term if sums[h] is None else sums[h] + term
        dn_mine[j // 2, j % 2] = added.astype(BF16)
    sums = [jnp.sum(term, 0, keepdims=True) for term in sums]
    blank = jnp.zeros((piece.shape[0] - HOP - 2, tile.shape[-1]), F32)
    piece[...] = jnp.concatenate([value[row_count : row_count + HOP], *sums, blank], 0)

    def beside():
        other = remote(dn_mine, dn_other, cs.at[1], cr.at[1], "chan", 1)
        other.start()
        other.wait()
        d_total = dn_mine[...].astype(F32) + dn_other[...].astype(F32)
        normal = standard[...]
        centred = d_total - jnp.mean(d_total, -1, keepdims=True)
        centred = centred - normal * jnp.mean(d_total * normal, -1, keepdims=True)
        grad[...] = (inverse[...] * centred).astype(BF16)

    gather_everywhere(piece, final, gzs, gzr, gxs, gxr, beside)
    arrived(pieces.at[pl.ds(0, 2 * (HOP - 1) * chain + 1)], ls)
    arrived(pieces.at[pl.ds(0, 2 * (chain - 1))], rs)


def call(kernel, name, identity, outs, scratch, *args):
    params = dict(vmem_limit_bytes=24 * 2**20)
    if identity is not None:
        params.update(collective_id=identity, has_side_effects=True)
    vmem = pl.BlockSpec(memory_space=pltpu.VMEM)
    return pl.pallas_call(
        kernel,
        out_shape=[jax.ShapeDtypeStruct(shape, kind) for shape, kind in outs],
        in_specs=[vmem] * len(args),
        out_specs=[vmem] * len(outs),
        scratch_shapes=scratch,
        compiler_params=pltpu.CompilerParams(**params),
        name=name,
    )(*args)


def on_device(pair_rep, pair_mask, w_qkvg, w_bias, w_out, cotangent):
    full_rows, block, channels = pair_rep.shape
    length, width = lax.axis_size("row"), lax.axis_size("col")
    cols = w_qkvg.shape[2]
    heads = w_bias.shape[1]
    scale = (cols // heads) ** (-0.5)
    own = full_rows // width
    tokens = width * block
    span = heads * block
    values = pair_rep.astype(F32)
    centred = values - jnp.mean(values, -1, keepdims=True)
    inverse = lax.rsqrt(jnp.mean(centred * centred, -1, keepdims=True) + EPSILON)
    standard = centred * inverse
    normed = standard.astype(BF16)
    piece = jnp.einsum("ijc,ch->ihj", normed, w_bias, preferred_element_type=F32)
    piece = piece.reshape(full_rows, span)
    mask = MASK_BIG * (pair_mask.astype(F32) - 1.0)
    mask = jnp.concatenate([mask, mask], 1).reshape(width, own, span)
    mask = jnp.pad(mask, ((0, 0), (0, 8 - own), (0, 0)))
    tiled = (width, own, block, channels)
    gathered = (width, length, full_rows, span)
    across = [DMA, DMA((length,)), DMA, DMA((width,))]
    bias, rows, cots, masks = call(
        gather_kernel,
        "gather",
        0,
        [(gathered, F32), (tiled, BF16), (tiled, BF16), (mask.shape, F32)],
        across + [DMA((3,)), DMA((3, width))],
        piece,
        normed.reshape(tiled),
        cotangent.reshape(tiled),
        mask,
    )
    wqk = jnp.concatenate([w_qkvg[0], w_qkvg[1]], 1)
    wvg = jnp.concatenate([w_qkvg[2], w_qkvg[3]], 1)
    grad_rows = 2 * channels + cols
    d_bias, upd, dn, grads = call(
        functools.partial(attend_kernel, scale),
        "attend",
        None,
        [
            ((width, tokens, span), BF16),
            (tiled, BF16),
            (tiled, BF16),
            ((width, grad_rows // width, channels), BF16),
        ],
        [],
        bias.reshape(width, tokens, span),
        rows,
        cots,
        masks,
        wqk,
        wvg,
        w_out,
    )
    V = pltpu.VMEM
    chain = length // 2 // HOP
    message = (2 * full_rows, span)
    tile, share = (V(tiled, BF16), V(grads.shape, BF16))
    relays = [V((chain, HOP - 1) + message, BF16)] * 2 + [V((chain,) + message, BF16)] * 4
    update, grad, final = call(
        reduce_kernel,
        "reduce",
        1,
        [(tiled, BF16), (tiled, BF16), (gathered, F32)],
        [V(d_bias.shape, BF16), share, tile, tile, tile, tile, tile]
        + [V((length,) + message, BF16)]
        + relays
        + [V((full_rows, span), F32)]
        + [DMA((4,)), DMA((4, width)), DMA]
        + [DMA((chain,))] * 4
        + [DMA, DMA((2,)), DMA((2,))]
        + across,
        d_bias,
        grads,
        upd,
        dn,
        standard.reshape(tiled),
        inverse.reshape(width, own, block, 1),
        w_bias.astype(F32).T,
    )
    used = grad_rows // width // HOP
    sums = final[:, :used, :HOP].reshape(grad_rows, channels) / tokens
    qkvg = sums[: 2 * channels].reshape(2, channels, 2, cols).transpose(0, 2, 1, 3)
    bias_grad = jnp.sum(final[:, :, HOP : HOP + heads], (0, 1)).T / tokens
    shape = pair_rep.shape
    return (
        update.reshape(shape),
        grad.reshape(shape),
        qkvg.reshape(w_qkvg.shape),
        bias_grad,
        sums[2 * channels :],
    )


def solution(mesh):
    in_specs = (
        P(("groups", "row"), "col", None),
        P(("groups", "row"), "col"),
        P(None, None, "chan"),
        P(None, "chan"),
        P("chan", None),
        P(("groups", "row"), "col", None),
    )
    out_specs = (
        P(("groups", "row"), "col", None),
        P(("groups", "row"), "col", None),
        P("groups", None, "chan"),
        P("groups", "chan"),
        P("chan", "groups"),
    )
    return jax.shard_map(
        on_device, mesh=mesh, in_specs=in_specs, out_specs=out_specs, check_vma=False
    )
```

```python
import functools

import jax
import jax.numpy as jnp
from jax import lax
from jax.experimental import pallas as pl
from jax.experimental.pallas import tpu as pltpu
from jax.sharding import PartitionSpec as P

EPSILON = 1e-05
MASK_BIG = 1000000000.0
MESH = pl.DeviceIdType.MESH
F32 = jnp.float32
BF16 = jnp.bfloat16
HOP = 4
DMA = pltpu.SemaphoreType.DMA


def place(axis, step):
    size = lax.axis_size(axis)
    return lax.rem(lax.axis_index(axis) + (step % size), size)


def remote(src, dst, send, recv, axis, step):
    return pltpu.make_async_remote_copy(
        src_ref=src,
        dst_ref=dst,
        send_sem=send,
        recv_sem=recv,
        device_id={axis: place(axis, step)},
        device_id_type=MESH,
    )


def arrived(dst, recv):
    pltpu.make_async_copy(dst, dst, recv).wait()


def gather_everywhere(piece, out, zs, zr, xs, xr, beside):
    length, width = lax.axis_size("row"), lax.axis_size("col")
    x, half = lax.axis_index("col"), length // 2
    last = half // HOP

    def slot_of(delta):
        return out.at[x, place("row", -delta)]

    def along_row(src, delta, steps):
        for step in steps:
            recv = zr.at[(delta + step) % length]
            remote(src, slot_of(delta), zs, recv, "row", step).start()

    def along_col(src, delta):
        for d in range(1, width):
            remote(src, slot_of(delta), xs, xr.at[d], "col", d).start()

    along_row(piece, 0, [s * t for t in (HOP, 3, 2, 1) for s in (1, -1)])
    along_col(piece, 0)
    out[x, lax.axis_index("row")] = piece[...]
    result = beside()
    for a in range(1, last + 1):
        for s in (1, -1):
            if a == last:
                continue
            delta = s * HOP * a
            arrived(slot_of(delta), zr.at[delta % length])
            far = [s * HOP] if (s == 1 or a < last - 1) else []
            along_row(slot_of(delta), delta, far + [s * t for t in (3, 2, 1)])
        for s in (1, -1):
            if a < last:
                along_col(slot_of(s * HOP * a), s * HOP * a)
            for t in range(1, HOP):
                delta = s * (HOP * (a - 1) + t)
                arrived(slot_of(delta), zr.at[delta % length])
                along_col(slot_of(delta), delta)
    arrived(slot_of(half), zr.at[half])
    along_col(slot_of(half), half)
    for d in range(1, width):
        arrived(out.at[place("col", -d)], xr.at[d])
    arrived(out.at[0, pl.ds(0, length - 1)], zs)
    arrived(out.at[pl.ds(0, width - 1)], xs)
    return result


def by_distance(length):
    return [s * t for t in range(1, length // 2) for s in (1, -1)] + [length // 2]


def to_all_rows(src_of, dst, send, recv_of):
    for step in reversed(by_distance(lax.axis_size("row"))):
        remote(src_of(step), dst, send, recv_of(step), "row", step).start()


def exchange(src, dst, xs, xr):
    for d in range(1, lax.axis_size("col")):
        remote(
            src.at[place("col", d)], dst.at[lax.axis_index("col")], xs, xr.at[d], "col", d
        ).start()


def exchanged(dst, xs, xr):
    for d in range(1, lax.axis_size("col")):
        arrived(dst.at[place("col", -d)], xr.at[d])
    arrived(dst.at[pl.ds(0, lax.axis_size("col") - 1)], xs)


def over(a, b):
    return lax.dot_general(a, b, (((1,), (1,)), ((), ())), preferred_element_type=F32)


def under(a, b):
    return lax.dot_general(a, b, (((0,), (0,)), ((), ())), preferred_element_type=F32)


def plain(a, b):
    return lax.dot_general(a, b, (((1,), (0,)), ((), ())), preferred_element_type=F32)


def standardized(values):
    values = values.astype(F32)
    centred = values - jnp.mean(values, -1, keepdims=True)
    inverse = lax.rsqrt(jnp.mean(centred * centred, -1, keepdims=True) + EPSILON)
    return centred * inverse, inverse


def add_up(values):
    return functools.reduce(jnp.add, values)


def whole_kernel(
    scale, pair, cot, mask, w_qkvg, w_bias, w_out, update, grad, share_all, bias_all,
    piece, bias, rows, cots, mask_own, masks, d_bias, bias_in, upd, upd_in, upd_other,
    dn, dn_in, dn_mine, dn_other, grads, grads_in, pieces, plus, minus, acc_plus, acc_minus,
    send_plus, send_minus, shares, shares_in, share_own, bias_own, bias_x, bias_row,
    gzs, gzr, gxs, gxr, es, er, bs, br, ls, lp, lm, ap, am, rs, cs, cr, ss, sr, fs, fr, fxs, fxr,
    ws, wr, vs, vr,
):
    length, width = lax.axis_size("row"), lax.axis_size("col")
    x, z = lax.axis_index("col"), lax.axis_index("row")
    _, row_count, block, channels = pair.shape
    cols = w_out.shape[0]
    size = cols // 2
    tokens, span, half = width * block, 2 * block, length // 2
    chain = half // HOP
    full_rows = width * row_count
    steps = [("chan", 1)] + [("col", d) for d in range(1, width)]
    steps += [("row", s * t) for t in range(1, HOP + 1) for s in (1, -1)]
    barrier = pltpu.get_barrier_semaphore()
    for axis, step in steps:
        pl.semaphore_signal(
            barrier, inc=1, device_id={axis: place(axis, step)}, device_id_type=MESH
        )

    standard, inverse = standardized(pair[...].reshape(full_rows * block, channels))
    normed_own = standard.astype(BF16)
    line = lax.broadcasted_iota(jnp.int32, (channels, channels), 0)
    eye = (line == lax.broadcasted_iota(jnp.int32, (channels, channels), 1)).astype(BF16)
    w_rows = under(w_bias[...], eye)
    flat = over(w_rows.astype(BF16), normed_own)
    lines = []
    for j in range(full_rows):
        part = flat[:, j * block : (j + 1) * block]
        lines += [jnp.concatenate([part[0:1], part[1:2]], 1)]
    piece[...] = jnp.concatenate(lines, 0)
    valid = MASK_BIG * (mask[...].astype(F32) - 1.0)
    mask_own[...] = jnp.concatenate([valid, valid], 1)
    wqk = jnp.concatenate([w_qkvg[0], w_qkvg[1]], 1)
    wvg = jnp.concatenate([w_qkvg[2], w_qkvg[3]], 1)
    pl.semaphore_wait(barrier, len(steps))

    head_lane = lax.broadcasted_iota(jnp.int32, (block, cols), 1) < size
    lane = lax.broadcasted_iota(jnp.int32, (tokens, span), 1) < block
    lane_col = lax.broadcasted_iota(jnp.int32, (tokens, cols), 1) < size

    def doubled(values):
        parts = []
        for n in range(width):
            part = values[n * block : (n + 1) * block]
            zero = jnp.zeros_like(part)
            parts += [jnp.where(head_lane, part, zero), jnp.where(head_lane, zero, part)]
        return jnp.concatenate(parts, 0)

    def halved(values):
        parts = []
        for n in range(width):
            first = values[n * span : n * span + block]
            second = values[n * span + block : (n + 1) * span]
            parts += [jnp.where(head_lane, first, second)]
        return jnp.concatenate(parts, 0)

    def per_head(parts, joined, reduced, empty):
        both = functools.reduce(joined, parts)
        first = reduced(jnp.where(lane, both, empty), axis=1, keepdims=True)
        second = reduced(jnp.where(lane, empty, both), axis=1, keepdims=True)
        return jnp.where(lane, first, second)

    def projections():
        exchange(pair, rows, es.at[0], er.at[0])
        exchange(cot, cots, es.at[1], er.at[1])
        for d in range(1, width):
            remote(mask_own, masks.at[x], es.at[2], er.at[2, d], "col", d).start()
        rows[x], cots[x], masks[x] = pair[x], cot[x], mask_own[...]
        for n, dst in enumerate((rows, cots, masks)):
            exchanged(dst, es.at[n], er.at[n])
        result = []
        for r in range(row_count):
            normed = standardized(rows[:, r].reshape(tokens, channels))[0].astype(BF16)
            row_cot = cots[:, r].reshape(tokens, channels)
            qk, vg = plain(normed, wqk), plain(normed, wvg)
            query = (qk[:, :cols] * scale).astype(BF16)
            key2 = doubled(qk[:, cols:]).astype(BF16)
            value2 = doubled(vg[:, :cols]).astype(BF16)
            gate = jax.nn.sigmoid(vg[:, cols:])
            d_gated = over(row_cot, w_out[...])
            d_attended = (d_gated * gate).astype(BF16)
            scores = over(query, key2)
            d_weights = over(d_attended, value2)
            result += [
                (normed, row_cot, query, key2, value2, gate, d_gated, d_attended, scores, d_weights)
            ]
        return result

    known = gather_everywhere(piece, bias, gzs, gzr, gxs, gxr, projections)

    bias_sum = [None] * width
    saved = []
    for r in range(row_count):
        _, _, _, _, value2, _, _, d_attended, scores, d_weights = known[r]
        parts = [
            (scores[:, n * span : (n + 1) * span] + bias[n].reshape(tokens, span))
            + masks[n, pl.ds(x * row_count + r, 1), :]
            for n in range(width)
        ]
        top = per_head(parts, jnp.maximum, jnp.max, -jnp.inf)
        parts = [jnp.exp(part - top) for part in parts]
        below = 1.0 / per_head(parts, jnp.add, jnp.sum, 0.0)
        weights = [part * below for part in parts]
        weights_b = jnp.concatenate([w.astype(BF16) for w in weights], 1)
        attended = plain(weights_b, value2)
        product = d_attended.astype(F32) * attended
        first = jnp.sum(jnp.where(lane_col, product, 0.0), axis=1, keepdims=True)
        second = jnp.sum(jnp.where(lane_col, 0.0, product), axis=1, keepdims=True)
        row_dot = jnp.where(lane, first, second)
        d_scores = [
            weights[n] * (d_weights[:, n * span : (n + 1) * span] - row_dot)
            for n in range(width)
        ]
        bias_sum = [d if b is None else b + d for b, d in zip(bias_sum, d_scores)]
        d_scores_b = jnp.concatenate([d.astype(BF16) for d in d_scores], 1)
        saved += [(weights_b, attended, d_scores_b)]
    for n in range(width):
        d_bias[n] = bias_sum[n].reshape(length, full_rows, span).astype(BF16)
    groups = []
    for a in range(chain):
        group = [s * (HOP * a + t) for t in range(1, HOP) for s in (1, -1)]
        group += [s * HOP * a for s in (1, -1)] if a else [0]
        groups += [group + [half] if a == chain - 1 else group]
    for a in range(chain - 1, -1, -1):
        for delta in groups[a]:
            dest = place("row", -delta)
            for d in range(1, width):
                remote(
                    d_bias.at[place("col", d), dest], bias_in.at[x, dest], bs, br.at[a, d], "col", d
                ).start()
    bias_in[x] = d_bias[x]

    gqk = gvg = gout = None
    for r in range(row_count):
        normed, row_cot, query, key2, _, gate, d_gated, d_attended, _, _ = known[r]
        weights_b, attended, d_scores_b = saved[r]
        gated = (gate * attended).astype(BF16)
        upd[:, r] = plain(gated, w_out[...]).astype(BF16).reshape(width, block, channels)
        d_gate = d_gated * attended * gate * (1.0 - gate)
        d_query = plain(d_scores_b, key2) * scale
        d_key = halved(under(d_scores_b, query))
        d_value = halved(under(weights_b, d_attended))
        dqk = jnp.concatenate([d_query, d_key], 1).astype(BF16)
        dvg = jnp.concatenate([d_value, d_gate], 1).astype(BF16)
        back = over(dqk, wqk) + over(dvg, wvg)
        dn[:, r] = back.astype(BF16).reshape(width, block, channels)
        new = (under(normed, dqk), under(normed, dvg), under(gated, row_cot))
        if gqk is None:
            gqk, gvg, gout = new
        else:
            gqk, gvg, gout = gqk + new[0], gvg + new[1], gout + new[2]
    part_rows = grads.shape[1]
    everything = jnp.concatenate([gqk, gvg, gout], 0).astype(BF16)
    for n in range(width):
        grads[n] = everything[n * part_rows : (n + 1) * part_rows]
    sources = ((grads, grads_in), (upd, upd_in), (dn, dn_in))
    for n, (src, dst) in enumerate(sources):
        exchange(src, dst, es.at[3 + n], er.at[3 + n])
    for src, dst in sources:
        dst[x] = src[x]

    sides = ((1, plus, acc_plus, send_plus, lp, ap), (-1, minus, acc_minus, send_minus, lm, am))
    for a in range(chain - 1, -1, -1):
        count = len(groups[a])
        for d in range(1, width):
            arrived(bias_in.at[0, pl.ds(0, count)], br.at[a, d])
        for delta in groups[a]:
            dest = place("row", -delta)
            pieces[dest] = add_up([bias_in[n, dest].astype(F32) for n in range(width)]).astype(BF16)
        if a == chain - 1:
            src = pieces.at[place("row", -half)]
            remote(src, acc_plus.at[a], ls, ap.at[a], "row", -HOP).start()
        for s, leaves, _, _, leaf_sem, _ in sides:
            for t in range(HOP - 1, 0, -1):
                src = pieces.at[place("row", -s * (t + HOP * a))]
                remote(src, leaves.at[a, t - 1], ls, leaf_sem.at[a], "row", -s * t).start()

    def relay(a):
        for s, leaves, acc, out, leaf_sem, acc_sem in sides:
            arrived(leaves.at[a], leaf_sem.at[a])
            value = pieces[place("row", -s * HOP * a)].astype(F32)
            value = value + add_up([leaves[a, t].astype(F32) for t in range(HOP - 1)])
            if s == 1 or a < chain - 1:
                arrived(acc.at[a], acc_sem.at[a])
                value = value + acc[a].astype(F32)
            out[a] = value.astype(BF16)
            remote(out.at[a], acc.at[a - 1], rs, acc_sem.at[a - 1], "row", -s * HOP).start()

    relay(chain - 1)
    exchanged(grads_in, es.at[3], er.at[3])
    summed = add_up([grads_in[n].astype(F32) for n in range(width)]).reshape(-1, HOP, channels)
    used = summed.shape[0]
    shares[pl.ds(0, used)] = summed.astype(BF16)
    shares[pl.ds(used, length - used)] = jnp.zeros((length - used, HOP, channels), BF16)
    to_all_rows(lambda step: shares.at[place("row", step)], shares_in.at[z], ss, lambda step: sr)
    for a in range(chain - 2, 0, -1):
        relay(a)
        if a == chain - 2:
            exchanged(upd_in, es.at[4], er.at[4])
            other = remote(upd_in, upd_other, cs.at[0], cr.at[0], "chan", 1)
            other.start()
            shares_in[z] = shares[z]
    other.wait()
    update[...] = (upd_in[...].astype(F32) + upd_other[...].astype(F32)).astype(BF16)
    exchanged(dn_in, es.at[5], er.at[5])
    tile = pieces[z].astype(F32)
    for s, leaves, acc, out, leaf_sem, acc_sem in sides:
        arrived(leaves.at[0], leaf_sem.at[0])
        arrived(acc.at[0], acc_sem.at[0])
        tile = tile + add_up([leaves[0, t].astype(F32) for t in range(HOP - 1)])
        tile = tile + acc[0].astype(F32)
    columns = jnp.transpose(tile)
    sums = [None, None]
    for j in range(full_rows):
        normed = normed_own[j * block : (j + 1) * block].astype(F32)
        added = dn_in[j // row_count, j % row_count].astype(F32)
        for h in range(2):
            column = columns[h * block : (h + 1) * block, j : j + 1]
            added = added + column * w_rows[h : h + 1, :]
            term = normed * column
            sums[h] = term if sums[h] is None else sums[h] + term
        dn_mine[j // row_count, j % row_count] = added.astype(BF16)
    sums = [jnp.sum(term, 0, keepdims=True) for term in sums]
    bias_own[...] = jnp.concatenate(sums, 0)
    for d in range(1, width):
        remote(bias_own, bias_x.at[x], ws, wr.at[d], "col", d).start()
    bias_x[x] = bias_own[...]
    other = remote(dn_mine, dn_other, cs.at[1], cr.at[1], "chan", 1)
    other.start()

    arrived(shares_in.at[pl.ds(0, length - 1)], sr)
    share_own[...] = jnp.sum(shares_in[...].astype(F32), 0).astype(BF16)
    to_all_rows(lambda step: share_own, share_all.at[x, z], fs, lambda step: fr.at[step % length])
    exchanged(bias_x, ws, wr)
    bias_row[...] = jnp.sum(bias_x[...], 0)
    to_all_rows(lambda step: bias_row, bias_all.at[z], vs, lambda step: vr)
    for d in range(1, width):
        remote(share_own, share_all.at[x, z], fxs, fxr.at[d], "col", d).start()
    share_all[x, z] = share_own[...]
    bias_all[z] = bias_row[...]

    other.wait()
    d_total = dn_mine[...].astype(F32) + dn_other[...].astype(F32)
    d_total = d_total.reshape(full_rows * block, channels)
    centred = d_total - jnp.mean(d_total, -1, keepdims=True)
    centred = centred - standard * jnp.mean(d_total * standard, -1, keepdims=True)
    grad[...] = (inverse * centred).astype(BF16).reshape(grad.shape)

    for step in by_distance(length):
        slot = share_all.at[x, place("row", -step)]
        arrived(slot, fr.at[step % length])
        for d in range(1, width):
            remote(slot, slot, fxs, fxr.at[d], "col", d).start()
    arrived(bias_all.at[pl.ds(0, length - 1)], vr)
    for d in range(1, width):
        arrived(share_all.at[place("col", -d)], fxr.at[d])
    for ref, sem in ((bias_all, vs), (share_all.at[0], fs), (shares, ss)):
        arrived(ref.at[pl.ds(0, length - 1)], sem)
    arrived(share_all.at[pl.ds(0, width - 1)], fxs)
    arrived(bias_in.at[pl.ds(0, width - 1)], bs)
    arrived(pieces.at[pl.ds(0, 2 * (HOP - 1) * chain + 1)], ls)
    arrived(pieces.at[pl.ds(0, 2 * (chain - 1))], rs)


def finish_kernel(tokens, update_in, grad_in, share_all, bias_all, update, grad, qkvg, bias, out):
    update[...] = update_in[...]
    grad[...] = grad_in[...]
    _, channels, cols = qkvg.shape
    total = 2 * channels + cols
    used = total // share_all.shape[0] // HOP
    rows = share_all[:, pl.ds(0, used)].astype(F32).reshape(total, channels) / tokens
    for p in range(2):
        part = rows[p * channels : (p + 1) * channels]
        qkvg[2 * p] = part[:, :cols]
        qkvg[2 * p + 1] = part[:, cols:]
    out[...] = rows[2 * channels :]
    both = jnp.sum(bias_all[...], 0) / tokens
    both = jnp.concatenate([both, jnp.zeros((6, channels), F32)], 0)
    bias[...] = jnp.transpose(both)[:, :2]


def call(kernel, name, identity, outs, scratch, *args):
    params = dict(vmem_limit_bytes=24 * 2**20)
    if identity is not None:
        params.update(collective_id=identity, has_side_effects=True)
    vmem = pl.BlockSpec(memory_space=pltpu.VMEM)
    return pl.pallas_call(
        kernel,
        out_shape=[jax.ShapeDtypeStruct(shape, kind) for shape, kind in outs],
        in_specs=[vmem] * len(args),
        out_specs=[vmem] * len(outs),
        scratch_shapes=scratch,
        compiler_params=pltpu.CompilerParams(**params),
        name=name,
    )(*args)


def on_device(pair_rep, pair_mask, w_qkvg, w_bias, w_out, cotangent):
    full_rows, block, channels = pair_rep.shape
    length, width = lax.axis_size("row"), lax.axis_size("col")
    cols = w_qkvg.shape[2]
    heads = w_bias.shape[1]
    scale = (cols // heads) ** (-0.5)
    tokens = width * block
    span = heads * block
    tiled = (width, full_rows // width, block, channels)
    part = (2 * channels + cols) // width
    chain = length // 2 // HOP
    message = (full_rows, span)
    V = pltpu.VMEM
    gathered = (width, length) + message
    share = (HOP, channels)
    tile = V(tiled, BF16)
    scratch = [V(message, F32), V(gathered, F32), tile, tile]
    scratch += [V(message, F32), V((width,) + message, F32)]
    scratch += [V(gathered, BF16)] * 2 + [tile] * 7
    scratch += [V((width, part, channels), BF16)] * 2 + [V((length,) + message, BF16)]
    scratch += [V((chain, HOP - 1) + message, BF16)] * 2 + [V((chain,) + message, BF16)] * 4
    scratch += [V((length,) + share, BF16)] * 2 + [V(share, BF16)]
    scratch += [V((heads, channels), F32), V((width, heads, channels), F32)]
    scratch += [V((heads, channels), F32)]
    scratch += [DMA, DMA((length,)), DMA, DMA((width,))]
    scratch += [DMA((6,)), DMA((6, width)), DMA, DMA((chain, width))]
    scratch += [DMA] + [DMA((chain,))] * 4 + [DMA, DMA((2,)), DMA((2,))]
    scratch += [DMA, DMA, DMA, DMA((length,)), DMA, DMA((width,))]
    scratch += [DMA, DMA((width,)), DMA, DMA]
    update, grad, share_all, bias_all = call(
        functools.partial(whole_kernel, scale),
        "whole",
        0,
        [
            (tiled, BF16),
            (tiled, BF16),
            ((width, length) + share, BF16),
            ((length, heads, channels), F32),
        ],
        scratch,
        pair_rep.reshape(tiled),
        cotangent.reshape(tiled),
        pair_mask,
        w_qkvg,
        w_bias,
        w_out,
    )
    shape = pair_rep.shape
    update, grad, qkvg, bias_grad, out = call(
        functools.partial(finish_kernel, tokens),
        "finish",
        None,
        [
            (tiled, BF16),
            (tiled, BF16),
            (w_qkvg.shape, F32),
            (w_bias.shape, F32),
            (w_out.shape, F32),
        ],
        [],
        update,
        grad,
        share_all,
        bias_all,
    )
    return (update.reshape(shape), grad.reshape(shape), qkvg, bias_grad, out)


def solution(mesh):
    in_specs = (
        P(("groups", "row"), "col", None),
        P(("groups", "row"), "col"),
        P(None, None, "chan"),
        P(None, "chan"),
        P("chan", None),
        P(("groups", "row"), "col", None),
    )
    out_specs = (
        P(("groups", "row"), "col", None),
        P(("groups", "row"), "col", None),
        P("groups", None, "chan"),
        P("groups", "chan"),
        P("chan", "groups"),
    )
    return jax.shard_map(
        on_device, mesh=mesh, in_specs=in_specs, out_specs=out_specs, check_vma=False
    )
```

```python
import functools

import jax
import jax.numpy as jnp
from jax import lax
from jax.experimental import pallas as pl
from jax.experimental.pallas import tpu as pltpu
from jax.sharding import PartitionSpec as P

EPSILON = 1e-05
MASK_BIG = 1000000000.0
MESH = pl.DeviceIdType.MESH
F32 = jnp.float32
BF16 = jnp.bfloat16
HOP = 4
DMA = pltpu.SemaphoreType.DMA


def place(axis, step):
    size = lax.axis_size(axis)
    return lax.rem(lax.axis_index(axis) + (step % size), size)


def remote(src, dst, send, recv, axis, step):
    return pltpu.make_async_remote_copy(
        src_ref=src,
        dst_ref=dst,
        send_sem=send,
        recv_sem=recv,
        device_id={axis: place(axis, step)},
        device_id_type=MESH,
    )


def arrived(dst, recv):
    pltpu.make_async_copy(dst, dst, recv).wait()


def gather_everywhere(piece, out, zs, zr, xs, xr, beside):
    length, width = lax.axis_size("row"), lax.axis_size("col")
    x, half = lax.axis_index("col"), length // 2
    last = half // HOP

    def slot_of(delta):
        return out.at[x, place("row", -delta)]

    def along_row(src, delta, steps):
        for step in steps:
            recv = zr.at[(delta + step) % length]
            remote(src, slot_of(delta), zs, recv, "row", step).start()

    def along_col(src, delta):
        for d in range(1, width):
            remote(src, slot_of(delta), xs, xr.at[d], "col", d).start()

    along_row(piece, 0, [s * t for t in (HOP, 3, 2, 1) for s in (1, -1)])
    along_col(piece, 0)
    out[x, lax.axis_index("row")] = piece[...]
    result = beside()
    for a in range(1, last + 1):
        for s in (1, -1):
            if a == last:
                continue
            delta = s * HOP * a
            arrived(slot_of(delta), zr.at[delta % length])
            far = [s * HOP] if (s == 1 or a < last - 1) else []
            along_row(slot_of(delta), delta, far + [s * t for t in (3, 2, 1)])
        for s in (1, -1):
            if a < last:
                along_col(slot_of(s * HOP * a), s * HOP * a)
            for t in range(1, HOP):
                delta = s * (HOP * (a - 1) + t)
                arrived(slot_of(delta), zr.at[delta % length])
                along_col(slot_of(delta), delta)
    arrived(slot_of(half), zr.at[half])
    along_col(slot_of(half), half)
    for d in range(1, width):
        arrived(out.at[place("col", -d)], xr.at[d])
    arrived(out.at[0, pl.ds(0, length - 1)], zs)
    arrived(out.at[pl.ds(0, width - 1)], xs)
    return result


def by_distance(length):
    return [s * t for t in range(1, length // 2) for s in (1, -1)] + [length // 2]


def to_all_rows(src_of, dst, send, recv_of):
    for step in reversed(by_distance(lax.axis_size("row"))):
        remote(src_of(step), dst, send, recv_of(step), "row", step).start()


def exchange(src, dst, xs, xr):
    for d in range(1, lax.axis_size("col")):
        remote(
            src.at[place("col", d)], dst.at[lax.axis_index("col")], xs, xr.at[d], "col", d
        ).start()


def exchanged(dst, xs, xr):
    for d in range(1, lax.axis_size("col")):
        arrived(dst.at[place("col", -d)], xr.at[d])
    arrived(dst.at[pl.ds(0, lax.axis_size("col") - 1)], xs)


def over(a, b):
    return lax.dot_general(a, b, (((1,), (1,)), ((), ())), preferred_element_type=F32)


def under(a, b):
    return lax.dot_general(a, b, (((0,), (0,)), ((), ())), preferred_element_type=F32)


def plain(a, b):
    return lax.dot_general(a, b, (((1,), (0,)), ((), ())), preferred_element_type=F32)


def standardized(values):
    values = values.astype(F32)
    centred = values - jnp.mean(values, -1, keepdims=True)
    inverse = lax.rsqrt(jnp.mean(centred * centred, -1, keepdims=True) + EPSILON)
    return centred * inverse, inverse


def add_up(values):
    return functools.reduce(jnp.add, values)


def whole_kernel(
    scale, pair_far, cot_far, mask_far, w_qkvg_far, w_bias_far, w_out_far, update, grad, share_all,
    bias_all, pair, cot, mask, w_qkvg, w_bias, w_out, piece, bias, rows, cots, mask_own, masks,
    d_bias, bias_in, upd, upd_in, upd_other, dn, dn_in, dn_mine, dn_other, grads, grads_in, pieces,
    tiles, shares, shares_in, share_own, bias_own, bias_x, bias_row, ins, gzs, gzr, gxs, gxr, es,
    er, bs, br, ls, lr, cs, cr, ss, sr, fs, fr, fxs, fxr, ws, wr, vs, vr,
):
    length, width = lax.axis_size("row"), lax.axis_size("col")
    x, z = lax.axis_index("col"), lax.axis_index("row")
    _, row_count, block, channels = pair.shape
    cols = w_out.shape[0]
    size = cols // 2
    tokens, span = width * block, 2 * block
    full_rows = width * row_count
    steps = [("chan", 1)] + [("col", d) for d in range(1, width)]
    steps += [("row", s * t) for t in range(1, HOP + 1) for s in (1, -1)]
    barrier = pltpu.get_barrier_semaphore()
    for axis, step in steps:
        pl.semaphore_signal(
            barrier, inc=1, device_id={axis: place(axis, step)}, device_id_type=MESH
        )

    loads = [
        pltpu.make_async_copy(src, dst, ins.at[n])
        for n, (src, dst) in enumerate(
            (
                (pair_far, pair),
                (w_bias_far, w_bias),
                (mask_far, mask),
                (w_qkvg_far, w_qkvg),
                (cot_far, cot),
                (w_out_far, w_out),
            )
        )
    ]
    for load in loads:
        load.start()
    for load in loads[:2]:
        load.wait()
    standard, inverse = standardized(pair[...].reshape(full_rows * block, channels))
    normed_own = standard.astype(BF16)
    w_rows = w_bias[...].astype(F32)
    flat = over(w_bias[...], normed_own)
    lines = []
    for j in range(full_rows):
        part = flat[:, j * block : (j + 1) * block]
        lines += [jnp.concatenate([part[0:1], part[1:2]], 1)]
    piece[...] = jnp.concatenate(lines, 0)
    for load in loads[2:]:
        load.wait()
    valid = MASK_BIG * (mask[...].astype(F32) - 1.0)
    mask_own[...] = jnp.concatenate([valid, valid], 1)
    wqk = jnp.concatenate([w_qkvg[0], w_qkvg[1]], 0)
    wvg = jnp.concatenate([w_qkvg[2], w_qkvg[3]], 0)
    pl.semaphore_wait(barrier, len(steps))

    head_lane = lax.broadcasted_iota(jnp.int32, (block, cols), 1) < size
    lane = lax.broadcasted_iota(jnp.int32, (tokens, span), 1) < block
    lane_col = lax.broadcasted_iota(jnp.int32, (tokens, cols), 1) < size

    def doubled(values):
        parts = []
        for n in range(width):
            part = values[n * block : (n + 1) * block]
            zero = jnp.zeros_like(part)
            parts += [jnp.where(head_lane, part, zero), jnp.where(head_lane, zero, part)]
        return jnp.concatenate(parts, 0)

    def halved(values):
        parts = []
        for n in range(width):
            first = values[n * span : n * span + block]
            second = values[n * span + block : (n + 1) * span]
            parts += [jnp.where(head_lane, first, second)]
        return jnp.concatenate(parts, 0)

    def per_head(parts, joined, reduced, empty):
        both = functools.reduce(joined, parts)
        first = reduced(jnp.where(lane, both, empty), axis=1, keepdims=True)
        second = reduced(jnp.where(lane, empty, both), axis=1, keepdims=True)
        return jnp.where(lane, first, second)

    def projections():
        exchange(pair, rows, es.at[0], er.at[0])
        exchange(cot, cots, es.at[1], er.at[1])
        for d in range(1, width):
            remote(mask_own, masks.at[x], es.at[2], er.at[2, d], "col", d).start()
        rows[x], cots[x], masks[x] = pair[x], cot[x], mask_own[...]
        for n, dst in enumerate((rows, cots, masks)):
            exchanged(dst, es.at[n], er.at[n])
        result = []
        for r in range(row_count):
            normed = standardized(rows[:, r].reshape(tokens, channels))[0].astype(BF16)
            row_cot = cots[:, r].reshape(tokens, channels)
            qk, vg = over(normed, wqk), over(normed, wvg)
            query = (qk[:, :cols] * scale).astype(BF16)
            key2 = doubled(qk[:, cols:]).astype(BF16)
            value2 = doubled(vg[:, :cols]).astype(BF16)
            gate = jax.nn.sigmoid(vg[:, cols:])
            d_gated = over(row_cot, w_out[...])
            d_attended = (d_gated * gate).astype(BF16)
            scores = over(query, key2)
            d_weights = over(d_attended, value2)
            result += [
                (normed, row_cot, query, key2, value2, gate, d_gated, d_attended, scores, d_weights)
            ]
        return result

    known = gather_everywhere(piece, bias, gzs, gzr, gxs, gxr, projections)

    bias_sum = [None] * width
    saved = []
    for r in range(row_count):
        _, _, _, _, value2, _, _, d_attended, scores, d_weights = known[r]
        parts = [
            (scores[:, n * span : (n + 1) * span] + bias[n].reshape(tokens, span))
            + masks[n, pl.ds(x * row_count + r, 1), :]
            for n in range(width)
        ]
        top = per_head(parts, jnp.maximum, jnp.max, -jnp.inf)
        parts = [jnp.exp(part - top) for part in parts]
        below = 1.0 / per_head(parts, jnp.add, jnp.sum, 0.0)
        weights = [part * below for part in parts]
        weights_b = jnp.concatenate([w.astype(BF16) for w in weights], 1)
        attended = plain(weights_b, value2)
        product = d_attended.astype(F32) * attended
        first = jnp.sum(jnp.where(lane_col, product, 0.0), axis=1, keepdims=True)
        second = jnp.sum(jnp.where(lane_col, 0.0, product), axis=1, keepdims=True)
        row_dot = jnp.where(lane, first, second)
        d_scores = [
            weights[n] * (d_weights[:, n * span : (n + 1) * span] - row_dot)
            for n in range(width)
        ]
        bias_sum = [d if b is None else b + d for b, d in zip(bias_sum, d_scores)]
        d_scores_b = jnp.concatenate([d.astype(BF16) for d in d_scores], 1)
        saved += [(weights_b, attended, d_scores_b)]
    for n in range(width):
        d_bias[n] = bias_sum[n].reshape(length, full_rows, span).astype(BF16)
    order = list(reversed([0] + by_distance(length)))
    quarter = length // 4
    groups = [order[n * quarter : (n + 1) * quarter] for n in range(4)]

    def send_group(n):
        for delta in groups[n]:
            dest = place("row", delta)
            for d in (2, 1, 3):
                src = d_bias.at[place("col", d), dest]
                remote(src, bias_in.at[x, dest], bs, br.at[n, d], "col", d).start()

    send_group(0)
    send_group(1)
    bias_in[x] = d_bias[x]

    gqk = gvg = gout = None
    for r in range(row_count):
        normed, row_cot, query, key2, _, gate, d_gated, d_attended, _, _ = known[r]
        weights_b, attended, d_scores_b = saved[r]
        gated = (gate * attended).astype(BF16)
        upd[:, r] = plain(gated, w_out[...]).astype(BF16).reshape(width, block, channels)
        d_gate = d_gated * attended * gate * (1.0 - gate)
        d_query = plain(d_scores_b, key2) * scale
        d_key = halved(under(d_scores_b, query))
        d_value = halved(under(weights_b, d_attended))
        dqk = jnp.concatenate([d_query, d_key], 1).astype(BF16)
        dvg = jnp.concatenate([d_value, d_gate], 1).astype(BF16)
        back = plain(dqk, wqk) + plain(dvg, wvg)
        dn[:, r] = back.astype(BF16).reshape(width, block, channels)
        new = (under(dqk, normed), under(dvg, normed), under(gated, row_cot))
        if gqk is None:
            gqk, gvg, gout = new
        else:
            gqk, gvg, gout = gqk + new[0], gvg + new[1], gout + new[2]
    part_rows = grads.shape[1]
    everything = jnp.concatenate([gqk, gvg, gout], 0).astype(BF16)
    for n in range(width):
        grads[n] = everything[n * part_rows : (n + 1) * part_rows]
    sources = ((grads, grads_in), (upd, upd_in), (dn, dn_in))
    exchange(grads, grads_in, es.at[3], er.at[3])
    send_group(2)
    send_group(3)
    exchange(dn, dn_in, es.at[5], er.at[5])
    exchange(upd, upd_in, es.at[4], er.at[4])
    for src, dst in sources:
        dst[x] = src[x]

    def send_tiles(n):
        for d in range(1, width):
            arrived(bias_in.at[0, pl.ds(0, quarter)], br.at[n, d])
        for delta in groups[n]:
            dest = place("row", delta)
            pieces[dest] = add_up([bias_in[m, dest].astype(F32) for m in range(width)]).astype(BF16)
        for delta in groups[n]:
            if delta:
                src = pieces.at[place("row", delta)]
                remote(src, tiles.at[z], ls, lr, "row", delta).start()

    send_tiles(0)
    send_tiles(1)
    exchanged(grads_in, es.at[3], er.at[3])
    summed = add_up([grads_in[n].astype(F32) for n in range(width)]).reshape(-1, HOP, channels)
    used = summed.shape[0]
    shares[pl.ds(0, used)] = summed.astype(BF16)
    shares[pl.ds(used, length - used)] = jnp.zeros((length - used, HOP, channels), BF16)
    to_all_rows(lambda step: shares.at[place("row", step)], shares_in.at[z], ss, lambda step: sr)
    send_tiles(2)
    send_tiles(3)
    tiles[z] = pieces[z]
    shares_in[z] = shares[z]
    exchanged(dn_in, es.at[5], er.at[5])
    exchanged(upd_in, es.at[4], er.at[4])
    other = remote(upd_in, upd_other, cs.at[0], cr.at[0], "chan", 1)
    other.start()
    other.wait()
    update[...] = (upd_in[...].astype(F32) + upd_other[...].astype(F32)).astype(BF16)
    arrived(tiles.at[pl.ds(0, length - 1)], lr)
    tile = jnp.sum(tiles[...].astype(F32), 0)
    columns = jnp.transpose(tile)
    sums = [None, None]
    for j in range(full_rows):
        normed = normed_own[j * block : (j + 1) * block].astype(F32)
        added = dn_in[j // row_count, j % row_count].astype(F32)
        for h in range(2):
            column = columns[h * block : (h + 1) * block, j : j + 1]
            added = added + column * w_rows[h : h + 1, :]
            term = normed * column
            sums[h] = term if sums[h] is None else sums[h] + term
        dn_mine[j // row_count, j % row_count] = added.astype(BF16)
    sums = [jnp.sum(term, 0, keepdims=True) for term in sums]
    bias_own[...] = jnp.concatenate(sums, 0)
    for d in range(1, width):
        remote(bias_own, bias_x.at[x], ws, wr.at[d], "col", d).start()
    bias_x[x] = bias_own[...]
    other = remote(dn_mine, dn_other, cs.at[1], cr.at[1], "chan", 1)
    other.start()

    exchanged(bias_x, ws, wr)
    bias_row[...] = jnp.sum(bias_x[...], 0)
    to_all_rows(lambda step: bias_row, bias_all.at[z], vs, lambda step: vr)
    arrived(shares_in.at[pl.ds(0, length - 1)], sr)
    share_own[...] = jnp.sum(shares_in[...].astype(F32), 0).astype(BF16)
    to_all_rows(lambda step: share_own, share_all.at[x, z], fs, lambda step: fr.at[step % length])
    for d in range(1, width):
        remote(share_own, share_all.at[x, z], fxs, fxr.at[d], "col", d).start()
    share_all[x, z] = share_own[...]
    bias_all[z] = bias_row[...]

    other.wait()
    d_total = dn_mine[...].astype(F32) + dn_other[...].astype(F32)
    d_total = d_total.reshape(full_rows * block, channels)
    centred = d_total - jnp.mean(d_total, -1, keepdims=True)
    centred = centred - standard * jnp.mean(d_total * standard, -1, keepdims=True)
    grad[...] = (inverse * centred).astype(BF16).reshape(grad.shape)

    for step in by_distance(length):
        slot = share_all.at[x, place("row", -step)]
        arrived(slot, fr.at[step % length])
        for d in range(1, width):
            remote(slot, slot, fxs, fxr.at[d], "col", d).start()
    arrived(bias_all.at[pl.ds(0, length - 1)], vr)
    for d in range(1, width):
        arrived(share_all.at[place("col", -d)], fxr.at[d])
    for ref, sem in ((bias_all, vs), (share_all.at[0], fs), (shares, ss)):
        arrived(ref.at[pl.ds(0, length - 1)], sem)
    arrived(share_all.at[pl.ds(0, width - 1)], fxs)
    arrived(bias_in.at[pl.ds(0, width - 1)], bs)
    arrived(pieces.at[pl.ds(0, length - 1)], ls)


def finish_kernel(tokens, update_in, grad_in, share_all, bias_all, update, grad, qkvg, bias, out):
    update[...] = update_in[...]
    grad[...] = grad_in[...]
    _, cols, channels = qkvg.shape
    total = 4 * cols + out.shape[0]
    used = total // share_all.shape[0] // HOP
    rows = share_all[:, pl.ds(0, used)].astype(F32).reshape(total, channels) / tokens
    qkvg[...] = rows[: 4 * cols].reshape(qkvg.shape)
    out[...] = rows[4 * cols :]
    bias[...] = jnp.sum(bias_all[...], 0) / tokens


def call(kernel, name, identity, outs, scratch, *args, near=pltpu.VMEM):
    params = dict(vmem_limit_bytes=60 * 2**20)
    if identity is not None:
        params.update(collective_id=identity, has_side_effects=True)
    vmem = pl.BlockSpec(memory_space=pltpu.VMEM)
    return pl.pallas_call(
        kernel,
        out_shape=[jax.ShapeDtypeStruct(shape, kind) for shape, kind in outs],
        in_specs=[pl.BlockSpec(memory_space=near)] * len(args),
        out_specs=[vmem] * len(outs),
        scratch_shapes=scratch,
        compiler_params=pltpu.CompilerParams(**params),
        name=name,
    )(*args)


def on_device(pair_rep, pair_mask, w_qkvg, w_bias, w_out, cotangent):
    full_rows, block, channels = pair_rep.shape
    length, width = lax.axis_size("row"), lax.axis_size("col")
    cols = w_qkvg.shape[2]
    heads = w_bias.shape[1]
    scale = (cols // heads) ** (-0.5)
    tokens = width * block
    span = heads * block
    tiled = (width, full_rows // width, block, channels)
    part = (2 * channels + cols) // width
    message = (full_rows, span)
    V = pltpu.VMEM
    gathered = (width, length) + message
    share = (HOP, channels)
    tile = V(tiled, BF16)
    stored = jnp.transpose(w_qkvg, (0, 2, 1))
    args = (
        pair_rep.reshape(tiled),
        cotangent.reshape(tiled),
        pair_mask,
        stored,
        w_bias.T,
        w_out,
    )
    scratch = [V(arg.shape, arg.dtype) for arg in args]
    scratch += [V(message, F32), V(gathered, F32), tile, tile]
    scratch += [V(message, F32), V((width,) + message, F32)]
    scratch += [V(gathered, BF16)] * 2 + [tile] * 7
    scratch += [V((width, part, channels), BF16)] * 2 + [V((length,) + message, BF16)] * 2
    scratch += [V((length,) + share, BF16)] * 2 + [V(share, BF16)]
    scratch += [V((heads, channels), F32), V((width, heads, channels), F32)]
    scratch += [V((heads, channels), F32)]
    scratch += [DMA((len(args),)), DMA, DMA((length,)), DMA, DMA((width,))]
    scratch += [DMA((6,)), DMA((6, width)), DMA, DMA((4, width))]
    scratch += [DMA, DMA, DMA((2,)), DMA((2,))]
    scratch += [DMA, DMA, DMA, DMA((length,)), DMA, DMA((width,))]
    scratch += [DMA, DMA((width,)), DMA, DMA]
    update, grad, share_all, bias_all = call(
        functools.partial(whole_kernel, scale),
        "whole",
        0,
        [
            (tiled, BF16),
            (tiled, BF16),
            ((width, length) + share, BF16),
            ((length, heads, channels), F32),
        ],
        scratch,
        *args,
        near=pltpu.HBM,
    )
    shape = pair_rep.shape
    update, grad, qkvg, bias_grad, out = call(
        functools.partial(finish_kernel, tokens),
        "finish",
        None,
        [
            (tiled, BF16),
            (tiled, BF16),
            (stored.shape, F32),
            (w_bias.T.shape, F32),
            (w_out.shape, F32),
        ],
        [],
        update,
        grad,
        share_all,
        bias_all,
    )
    qkvg = jnp.transpose(qkvg, (0, 2, 1))
    return (update.reshape(shape), grad.reshape(shape), qkvg, bias_grad.T, out)


def solution(mesh):
    in_specs = (
        P(("groups", "row"), "col", None),
        P(("groups", "row"), "col"),
        P(None, None, "chan"),
        P(None, "chan"),
        P("chan", None),
        P(("groups", "row"), "col", None),
    )
    out_specs = (
        P(("groups", "row"), "col", None),
        P(("groups", "row"), "col", None),
        P("groups", None, "chan"),
        P("groups", "chan"),
        P("chan", "groups"),
    )
    return jax.shard_map(
        on_device, mesh=mesh, in_specs=in_specs, out_specs=out_specs, check_vma=False
    )
```

```python
import functools

import jax
import jax.numpy as jnp
from jax import lax
from jax.experimental import pallas as pl
from jax.experimental.pallas import tpu as pltpu
from jax.sharding import PartitionSpec as P

EPSILON = 1e-05
MASK_BIG = 1000000000.0
MESH = pl.DeviceIdType.MESH
F32 = jnp.float32
BF16 = jnp.bfloat16
HOP = 4
DMA = pltpu.SemaphoreType.DMA


def place(axis, step):
    size = lax.axis_size(axis)
    return lax.rem(lax.axis_index(axis) + (step % size), size)


def remote(src, dst, send, recv, axis, step):
    return pltpu.make_async_remote_copy(
        src_ref=src,
        dst_ref=dst,
        send_sem=send,
        recv_sem=recv,
        device_id={axis: place(axis, step)},
        device_id_type=MESH,
    )


def arrived(dst, recv):
    pltpu.make_async_copy(dst, dst, recv).wait()


def gather_everywhere(piece, out, zs, zr, xs, xr, gaps):
    length, width = lax.axis_size("row"), lax.axis_size("col")
    x, half = lax.axis_index("col"), length // 2
    last = half // HOP

    def along_row(src, delta, steps):
        for step in steps:
            k = (delta + step) % length
            remote(src, out.at[x, k], zs, zr.at[k], "row", step).start()

    def along_col(src, first, count):
        slots = out.at[x, pl.ds(first, count)]
        for d in (2, 1, 3):
            remote(slots if src is None else src, slots, xs, xr.at[d], "col", d).start()

    def wait(delta):
        arrived(out.at[x, delta % length], zr.at[delta % length])

    along_row(piece.at[0], 0, [s * t for t in (HOP, 3, 2, 1) for s in (1, -1)])
    along_col(piece, 0, 1)
    out[x, 0] = piece[0]
    gaps[0]()
    for a in range(1, last):
        for s in (1, -1):
            wait(s * HOP * a)
            far = [s * HOP] if (s == 1 or a < last - 1) else []
            along_row(out.at[x, s * HOP * a % length], s * HOP * a, far + [s * t for t in (3, 2, 1)])
        for s in (1, -1):
            for t in range(1, HOP):
                wait(s * (HOP * (a - 1) + t))
            along_col(None, HOP * (a - 1) + 1 if s == 1 else length - HOP * a, HOP)
        gaps[a]()
    for t in range(1, HOP):
        for s in (1, -1):
            wait(s * (half - HOP + t))
    along_col(None, half + 1, HOP - 1)
    along_col(None, half - HOP + 1, HOP - 1)
    wait(half)
    along_col(None, half, 1)
    for d in range(1, width):
        arrived(out.at[place("col", -d)], xr.at[d])
    arrived(out.at[0, pl.ds(0, length - 1)], zs)
    arrived(out.at[pl.ds(0, width - 1)], xs)


def by_distance(length):
    return [s * t for t in range(1, length // 2) for s in (1, -1)] + [length // 2]


def to_all_rows(src_of, dst_of, send, recv_of):
    for step in reversed(by_distance(lax.axis_size("row"))):
        remote(src_of(step), dst_of(step), send, recv_of(step), "row", step).start()


def exchange(src, dst, xs, xr):
    for d in range(1, lax.axis_size("col")):
        remote(
            src.at[place("col", d)], dst.at[lax.axis_index("col")], xs, xr.at[d], "col", d
        ).start()


def exchanged(dst, xs, xr):
    for d in range(1, lax.axis_size("col")):
        arrived(dst.at[place("col", -d)], xr.at[d])
    arrived(dst.at[pl.ds(0, lax.axis_size("col") - 1)], xs)


def over(a, b):
    return lax.dot_general(a, b, (((1,), (1,)), ((), ())), preferred_element_type=F32)


def under(a, b):
    return lax.dot_general(a, b, (((0,), (0,)), ((), ())), preferred_element_type=F32)


def plain(a, b):
    return lax.dot_general(a, b, (((1,), (0,)), ((), ())), preferred_element_type=F32)


def standardized(values):
    values = values.astype(F32)
    centred = values - jnp.mean(values, -1, keepdims=True)
    inverse = lax.rsqrt(jnp.mean(centred * centred, -1, keepdims=True) + EPSILON)
    return centred * inverse, inverse


def add_up(values):
    return functools.reduce(jnp.add, values)


def whole_kernel(
    scale, pair_far, cot_far, mask_far, w_qkvg_far, w_bias_far, w_out_far, update, grad, share_all,
    bias_all, pair, cot, mask, w_qkvg, w_bias, w_out, piece, bias, rows, cots, mask_own, masks,
    d_bias, bias_in, upd, upd_in, upd_other, dn, dn_in, dn_mine, dn_other, grads, grads_in, pieces,
    tiles, shares, shares_in, share_own, bias_own, bias_x, bias_row, ins, gzs, gzr, gxs, gxr, es,
    er, rs, rr, hs, hr, bs, br, ls, lr, cs, cr, ss, sr, fs, fr, fxs, fxr, ws, wr, vs, vr,
):
    length, width = lax.axis_size("row"), lax.axis_size("col")
    x, z = lax.axis_index("col"), lax.axis_index("row")
    _, row_count, block, channels = pair.shape
    cols = w_out.shape[0]
    size = cols // 2
    tokens, span = width * block, 2 * block
    full_rows = width * row_count
    steps = [("chan", 1)] + [("col", d) for d in range(1, width)]
    steps += [("row", s * t) for t in range(1, HOP + 1) for s in (1, -1)]
    barrier = pltpu.get_barrier_semaphore()
    for axis, step in steps:
        pl.semaphore_signal(
            barrier, inc=1, device_id={axis: place(axis, step)}, device_id_type=MESH
        )

    loads = [
        pltpu.make_async_copy(src, dst, ins.at[n])
        for n, (src, dst) in enumerate(
            (
                (pair_far, pair),
                (w_bias_far, w_bias),
                (mask_far, mask),
                (w_qkvg_far, w_qkvg),
                (cot_far, cot),
                (w_out_far, w_out),
            )
        )
    ]
    for load in loads:
        load.start()
    for load in loads[:2]:
        load.wait()
    standard, inverse = standardized(pair[...].reshape(full_rows * block, channels))
    normed_own = standard.astype(BF16)
    w_rows = w_bias[...].astype(F32)
    flat = over(w_bias[...], normed_own)
    lines = []
    for j in range(full_rows):
        part = flat[:, j * block : (j + 1) * block]
        lines += [jnp.concatenate([part[0:1], part[1:2]], 1)]
    piece[0] = jnp.concatenate(lines, 0)
    for load in loads[2:]:
        load.wait()
    valid = MASK_BIG * (mask[...].astype(F32) - 1.0)
    mask_own[...] = jnp.concatenate([valid, valid], 1)
    wqk = jnp.concatenate([w_qkvg[0], w_qkvg[1]], 0)
    wvg = jnp.concatenate([w_qkvg[2], w_qkvg[3]], 0)
    pl.semaphore_wait(barrier, len(steps))

    head_lane = lax.broadcasted_iota(jnp.int32, (block, cols), 1) < size
    lane = lax.broadcasted_iota(jnp.int32, (tokens, span), 1) < block
    lane_col = lax.broadcasted_iota(jnp.int32, (tokens, cols), 1) < size

    def doubled(values):
        parts = []
        for n in range(width):
            part = values[n * block : (n + 1) * block]
            zero = jnp.zeros_like(part)
            parts += [jnp.where(head_lane, part, zero), jnp.where(head_lane, zero, part)]
        return jnp.concatenate(parts, 0)

    def halved(values):
        parts = []
        for n in range(width):
            first = values[n * span : n * span + block]
            second = values[n * span + block : (n + 1) * span]
            parts += [jnp.where(head_lane, first, second)]
        return jnp.concatenate(parts, 0)

    def per_head(parts, joined, reduced, empty):
        both = functools.reduce(joined, parts)
        first = reduced(jnp.where(lane, both, empty), axis=1, keepdims=True)
        second = reduced(jnp.where(lane, empty, both), axis=1, keepdims=True)
        return jnp.where(lane, first, second)

    core = lax.axis_index("chan")
    halves = ((pair, rows), (cot, cots))
    known = []

    def start_exchange():
        for n, (src, dst) in enumerate(halves):
            for d in (2, 1, 3):
                half = src.at[place("col", d), core]
                remote(half, dst.at[x, core], rs.at[n, d], rr.at[n, d], "col", d).start()
        for d in (2, 1, 3):
            remote(mask_own, masks.at[x], es.at[2], er.at[2, d], "col", d).start()
        rows[x], cots[x], masks[x] = pair[x], cot[x], mask_own[...]

    def hand_over():
        for n, (src, dst) in enumerate(halves):
            for d in range(1, width):
                half = dst.at[place("col", -d), core]
                arrived(half, rr.at[n, d])
                remote(half, half, hs.at[n, d], hr.at[n, d], "chan", 1).start()
        for n, (src, dst) in enumerate(halves):
            for d in range(1, width):
                arrived(src.at[0, 0], rs.at[n, d])

    def project(r):
        normed = standardized(rows[:, r].reshape(tokens, channels))[0].astype(BF16)
        row_cot = cots[:, r].reshape(tokens, channels)
        qk, vg = over(normed, wqk), over(normed, wvg)
        query = (qk[:, :cols] * scale).astype(BF16)
        key2 = doubled(qk[:, cols:]).astype(BF16)
        value2 = doubled(vg[:, :cols]).astype(BF16)
        gate = jax.nn.sigmoid(vg[:, cols:])
        d_gated = over(row_cot, w_out[...])
        d_attended = (d_gated * gate).astype(BF16)
        scores = over(query, key2)
        d_weights = over(d_attended, value2)
        known.append(
            (normed, row_cot, query, key2, value2, gate, d_gated, d_attended, scores, d_weights)
        )

    def first_row():
        for n, (_, dst) in enumerate(halves):
            for d in range(1, width):
                arrived(dst.at[place("col", -d), 1 - core], hr.at[n, d])
                arrived(dst.at[0, 0], hs.at[n, d])
        exchanged(masks, es.at[2], er.at[2])
        project(0)

    def other_rows():
        for r in range(1, row_count):
            project(r)

    gaps = (start_exchange, hand_over, first_row, other_rows)
    gather_everywhere(piece, bias, gzs, gzr, gxs, gxr, gaps)
    blocks = [lax.rem(z + length - b, length) for b in range(length)]

    bias_sum = [None] * width
    saved = []
    for r in range(row_count):
        _, _, _, _, value2, _, _, d_attended, scores, d_weights = known[r]
        parts = [
            (scores[:, n * span : (n + 1) * span] + jnp.concatenate([bias[n, k] for k in blocks], 0))
            + masks[n, pl.ds(x * row_count + r, 1), :]
            for n in range(width)
        ]
        top = per_head(parts, jnp.maximum, jnp.max, -jnp.inf)
        parts = [jnp.exp(part - top) for part in parts]
        below = 1.0 / per_head(parts, jnp.add, jnp.sum, 0.0)
        weights = [part * below for part in parts]
        weights_b = jnp.concatenate([w.astype(BF16) for w in weights], 1)
        attended = plain(weights_b, value2)
        product = d_attended.astype(F32) * attended
        first = jnp.sum(jnp.where(lane_col, product, 0.0), axis=1, keepdims=True)
        second = jnp.sum(jnp.where(lane_col, 0.0, product), axis=1, keepdims=True)
        row_dot = jnp.where(lane, first, second)
        d_scores = [
            weights[n] * (d_weights[:, n * span : (n + 1) * span] - row_dot)
            for n in range(width)
        ]
        bias_sum = [d if b is None else b + d for b, d in zip(bias_sum, d_scores)]
        d_scores_b = jnp.concatenate([d.astype(BF16) for d in d_scores], 1)
        saved += [(weights_b, attended, d_scores_b)]
    for n in range(width):
        for b in range(length):
            part = bias_sum[n][b * full_rows : (b + 1) * full_rows]
            d_bias[n, lax.rem(b + length - z, length)] = part.astype(BF16)
    quarter, half = length // 4, length // 2
    step = quarter // 2
    groups = [((half - step, quarter),)]
    groups += [((half - n * step, step), (half + (n - 1) * step, step)) for n in range(2, 5)]

    def send_group(n):
        for first, count in groups[n]:
            slots = pl.ds(first, count)
            for d in (2, 1, 3):
                src = d_bias.at[place("col", d), slots]
                remote(src, bias_in.at[x, slots], bs, br.at[n, d], "col", d).start()

    send_group(0)
    send_group(1)
    bias_in[x] = d_bias[x]

    gqk = gvg = gout = None
    for r in range(row_count):
        normed, row_cot, query, key2, _, gate, d_gated, d_attended, _, _ = known[r]
        weights_b, attended, d_scores_b = saved[r]
        gated = (gate * attended).astype(BF16)
        upd[:, r] = plain(gated, w_out[...]).astype(BF16).reshape(width, block, channels)
        d_gate = d_gated * attended * gate * (1.0 - gate)
        d_query = plain(d_scores_b, key2) * scale
        d_key = halved(under(d_scores_b, query))
        d_value = halved(under(weights_b, d_attended))
        dqk = jnp.concatenate([d_query, d_key], 1).astype(BF16)
        dvg = jnp.concatenate([d_value, d_gate], 1).astype(BF16)
        back = plain(dqk, wqk) + plain(dvg, wvg)
        dn[:, r] = back.astype(BF16).reshape(width, block, channels)
        new = (under(dqk, normed), under(dvg, normed), under(gated, row_cot))
        if gqk is None:
            gqk, gvg, gout = new
        else:
            gqk, gvg, gout = gqk + new[0], gvg + new[1], gout + new[2]
    part_rows = grads.shape[1]
    everything = jnp.concatenate([gqk, gvg, gout], 0).astype(BF16)
    for n in range(width):
        grads[n] = everything[n * part_rows : (n + 1) * part_rows]
    sources = ((grads, grads_in), (upd, upd_in), (dn, dn_in))
    exchange(grads, grads_in, es.at[3], er.at[3])
    send_group(2)
    send_group(3)
    exchange(dn, dn_in, es.at[5], er.at[5])
    exchange(upd, upd_in, es.at[4], er.at[4])
    for src, dst in sources:
        dst[x] = src[x]

    def send_tiles(n):
        for d in range(1, width):
            arrived(bias_in.at[0, pl.ds(0, quarter)], br.at[n, d])
        slots = []
        for first, count in groups[n]:
            parts = [bias_in[m, first : first + count].astype(F32) for m in range(width)]
            pieces[first : first + count] = add_up(parts).astype(BF16)
            slots += range(first, first + count)
        for k in sorted(slots, key=lambda k: -min(k, length - k)):
            if k:
                remote(pieces.at[k], tiles.at[k], ls, lr, "row", k).start()

    send_tiles(0)
    send_tiles(1)
    exchanged(grads_in, es.at[3], er.at[3])
    summed = add_up([grads_in[n].astype(F32) for n in range(width)]).reshape(-1, HOP, channels)
    used = summed.shape[0]
    shares[pl.ds(0, used)] = summed.astype(BF16)
    shares[pl.ds(used, length - used)] = jnp.zeros((length - used, HOP, channels), BF16)
    to_all_rows(
        lambda step: shares.at[place("row", step)],
        lambda step: shares_in.at[step % length],
        ss,
        lambda step: sr,
    )
    send_tiles(2)
    send_tiles(3)
    tiles[0] = pieces[0]
    shares_in[0] = shares[z]
    exchanged(dn_in, es.at[5], er.at[5])
    exchanged(upd_in, es.at[4], er.at[4])
    other = remote(upd_in, upd_other, cs.at[0], cr.at[0], "chan", 1)
    other.start()
    other.wait()
    update[...] = (upd_in[...].astype(F32) + upd_other[...].astype(F32)).astype(BF16)
    arrived(tiles.at[pl.ds(0, length - 1)], lr)
    tile = jnp.sum(tiles[...].astype(F32), 0)
    columns = jnp.transpose(tile)
    sums = [None, None]
    for j in range(full_rows):
        normed = normed_own[j * block : (j + 1) * block].astype(F32)
        for h in range(2):
            term = normed * columns[h * block : (h + 1) * block, j : j + 1]
            sums[h] = term if sums[h] is None else sums[h] + term
    sums = [jnp.sum(term, 0, keepdims=True) for term in sums]
    bias_own[...] = jnp.concatenate(sums, 0)
    for d in (2, 1, 3):
        remote(bias_own, bias_x.at[x], ws, wr.at[d], "col", d).start()
    bias_x[x] = bias_own[...]
    for j in range(full_rows):
        added = dn_in[j // row_count, j % row_count].astype(F32)
        for h in range(2):
            column = columns[h * block : (h + 1) * block, j : j + 1]
            added = added + column * w_rows[h : h + 1, :]
        dn_mine[j // row_count, j % row_count] = added.astype(BF16)
    other = remote(dn_mine, dn_other, cs.at[1], cr.at[1], "chan", 1)
    other.start()

    arrived(shares_in.at[pl.ds(0, length - 1)], sr)
    share_own[...] = jnp.sum(shares_in[...].astype(F32), 0).astype(BF16)
    to_all_rows(
        lambda step: share_own,
        lambda step: share_all.at[x, z],
        fs,
        lambda step: fr.at[step % length],
    )
    exchanged(bias_x, ws, wr)
    bias_row[...] = jnp.sum(bias_x[...], 0)
    to_all_rows(
        lambda step: bias_row, lambda step: bias_all.at[step % length], vs, lambda step: vr
    )
    for d in range(1, width):
        remote(share_own, share_all.at[x, z], fxs, fxr.at[d], "col", d).start()
    share_all[x, z] = share_own[...]
    bias_all[0] = bias_row[...]

    other.wait()
    d_total = dn_mine[...].astype(F32) + dn_other[...].astype(F32)
    d_total = d_total.reshape(full_rows * block, channels)
    centred = d_total - jnp.mean(d_total, -1, keepdims=True)
    centred = centred - standard * jnp.mean(d_total * standard, -1, keepdims=True)
    grad[...] = (inverse * centred).astype(BF16).reshape(grad.shape)

    for step in by_distance(length):
        slot = share_all.at[x, place("row", -step)]
        arrived(slot, fr.at[step % length])
        for d in range(1, width):
            remote(slot, slot, fxs, fxr.at[d], "col", d).start()
    arrived(bias_all.at[pl.ds(0, length - 1)], vr)
    for d in range(1, width):
        arrived(share_all.at[place("col", -d)], fxr.at[d])
    for ref, sem in ((bias_all, vs), (share_all.at[0], fs), (shares, ss)):
        arrived(ref.at[pl.ds(0, length - 1)], sem)
    arrived(share_all.at[pl.ds(0, width - 1)], fxs)
    arrived(bias_in.at[pl.ds(0, width - 1)], bs)
    arrived(pieces.at[pl.ds(0, length - 1)], ls)


def finish_kernel(tokens, update_in, grad_in, share_all, bias_all, update, grad, qkvg, bias, out):
    update[...] = update_in[...]
    grad[...] = grad_in[...]
    _, cols, channels = qkvg.shape
    total = 4 * cols + out.shape[0]
    used = total // share_all.shape[0] // HOP
    rows = share_all[:, pl.ds(0, used)].astype(F32).reshape(total, channels) / tokens
    qkvg[...] = rows[: 4 * cols].reshape(qkvg.shape)
    out[...] = rows[4 * cols :]
    bias[...] = jnp.sum(bias_all[...], 0) / tokens


def call(kernel, name, identity, outs, scratch, *args, near=pltpu.VMEM):
    params = dict(vmem_limit_bytes=60 * 2**20)
    if identity is not None:
        params.update(collective_id=identity, has_side_effects=True)
    vmem = pl.BlockSpec(memory_space=pltpu.VMEM)
    return pl.pallas_call(
        kernel,
        out_shape=[jax.ShapeDtypeStruct(shape, kind) for shape, kind in outs],
        in_specs=[pl.BlockSpec(memory_space=near)] * len(args),
        out_specs=[vmem] * len(outs),
        scratch_shapes=scratch,
        compiler_params=pltpu.CompilerParams(**params),
        name=name,
    )(*args)


def on_device(pair_rep, pair_mask, w_qkvg, w_bias, w_out, cotangent):
    full_rows, block, channels = pair_rep.shape
    length, width = lax.axis_size("row"), lax.axis_size("col")
    cols = w_qkvg.shape[2]
    heads = w_bias.shape[1]
    scale = (cols // heads) ** (-0.5)
    tokens = width * block
    span = heads * block
    tiled = (width, full_rows // width, block, channels)
    part = (2 * channels + cols) // width
    message = (full_rows, span)
    V = pltpu.VMEM
    gathered = (width, length) + message
    share = (HOP, channels)
    tile = V(tiled, BF16)
    stored = jnp.transpose(w_qkvg, (0, 2, 1))
    args = (
        pair_rep.reshape(tiled),
        cotangent.reshape(tiled),
        pair_mask,
        stored,
        w_bias.T,
        w_out,
    )
    scratch = [V(arg.shape, arg.dtype) for arg in args]
    scratch += [V((1,) + message, F32), V(gathered, F32), tile, tile]
    scratch += [V(message, F32), V((width,) + message, F32)]
    scratch += [V(gathered, BF16)] * 2 + [tile] * 7
    scratch += [V((width, part, channels), BF16)] * 2 + [V((length,) + message, BF16)] * 2
    scratch += [V((length,) + share, BF16)] * 2 + [V(share, BF16)]
    scratch += [V((heads, channels), F32), V((width, heads, channels), F32)]
    scratch += [V((heads, channels), F32)]
    scratch += [DMA((len(args),)), DMA, DMA((length,)), DMA, DMA((width,))]
    scratch += [DMA((6,)), DMA((6, width))] + [DMA((2, width))] * 4 + [DMA, DMA((4, width))]
    scratch += [DMA, DMA, DMA((2,)), DMA((2,))]
    scratch += [DMA, DMA, DMA, DMA((length,)), DMA, DMA((width,))]
    scratch += [DMA, DMA((width,)), DMA, DMA]
    update, grad, share_all, bias_all = call(
        functools.partial(whole_kernel, scale),
        "whole",
        0,
        [
            (tiled, BF16),
            (tiled, BF16),
            ((width, length) + share, BF16),
            ((length, heads, channels), F32),
        ],
        scratch,
        *args,
        near=pltpu.HBM,
    )
    shape = pair_rep.shape
    update, grad, qkvg, bias_grad, out = call(
        functools.partial(finish_kernel, tokens),
        "finish",
        None,
        [
            (tiled, BF16),
            (tiled, BF16),
            (stored.shape, F32),
            (w_bias.T.shape, F32),
            (w_out.shape, F32),
        ],
        [],
        update,
        grad,
        share_all,
        bias_all,
    )
    qkvg = jnp.transpose(qkvg, (0, 2, 1))
    return (update.reshape(shape), grad.reshape(shape), qkvg, bias_grad.T, out)


def solution(mesh):
    in_specs = (
        P(("groups", "row"), "col", None),
        P(("groups", "row"), "col"),
        P(None, None, "chan"),
        P(None, "chan"),
        P("chan", None),
        P(("groups", "row"), "col", None),
    )
    out_specs = (
        P(("groups", "row"), "col", None),
        P(("groups", "row"), "col", None),
        P("groups", None, "chan"),
        P("groups", "chan"),
        P("chan", "groups"),
    )
    return jax.shard_map(
        on_device, mesh=mesh, in_specs=in_specs, out_specs=out_specs, check_vma=False
    )
```

```python
import functools

import jax
import jax.numpy as jnp
from jax import lax
from jax.experimental import pallas as pl
from jax.experimental.pallas import tpu as pltpu
from jax.sharding import PartitionSpec as P

EPSILON = 1e-05
MASK_BIG = 1000000000.0
MESH = pl.DeviceIdType.MESH
F32 = jnp.float32
BF16 = jnp.bfloat16
HOP = 4
DMA = pltpu.SemaphoreType.DMA


def place(axis, step):
    size = lax.axis_size(axis)
    return lax.rem(lax.axis_index(axis) + (step % size), size)


def remote(src, dst, send, recv, axis, step):
    return pltpu.make_async_remote_copy(
        src_ref=src,
        dst_ref=dst,
        send_sem=send,
        recv_sem=recv,
        device_id={axis: place(axis, step)},
        device_id_type=MESH,
    )


def arrived(dst, recv):
    pltpu.make_async_copy(dst, dst, recv).wait()


def gather_everywhere(piece, out, zs, zr, xs, xr, gaps):
    length, width = lax.axis_size("row"), lax.axis_size("col")
    x, half = lax.axis_index("col"), length // 2
    last = half // HOP

    def along_row(src, delta, steps):
        for step in steps:
            k = (delta + step) % length
            remote(src, out.at[x, k], zs, zr.at[k], "row", step).start()

    def along_col(src, first, count):
        slots = out.at[x, pl.ds(first, count)]
        for d in (2, 1, 3):
            remote(slots if src is None else src, slots, xs, xr.at[d], "col", d).start()

    def wait(delta):
        arrived(out.at[x, delta % length], zr.at[delta % length])

    along_row(piece.at[0], 0, [s * t for t in (HOP, 3, 2, 1) for s in (1, -1)])
    along_col(piece, 0, 1)
    out[x, 0] = piece[0]
    gaps[0]()
    for a in range(1, last):
        for s in (1, -1):
            wait(s * HOP * a)
            far = [s * HOP] if (s == 1 or a < last - 1) else []
            along_row(out.at[x, s * HOP * a % length], s * HOP * a, far + [s * t for t in (3, 2, 1)])
        for s in (1, -1):
            for t in range(1, HOP):
                wait(s * (HOP * (a - 1) + t))
            along_col(None, HOP * (a - 1) + 1 if s == 1 else length - HOP * a, HOP)
        gaps[a]()
    for t in range(1, HOP):
        for s in (1, -1):
            wait(s * (half - HOP + t))
    along_col(None, half + 1, HOP - 1)
    along_col(None, half - HOP + 1, HOP - 1)
    wait(half)
    along_col(None, half, 1)
    for d in range(1, width):
        arrived(out.at[place("col", -d)], xr.at[d])
    arrived(out.at[0, pl.ds(0, length - 1)], zs)
    arrived(out.at[pl.ds(0, width - 1)], xs)


def by_distance(length):
    return [s * t for t in range(1, length // 2) for s in (1, -1)] + [length // 2]


def to_all_rows(src_of, dst_of, send, recv_of):
    for step in reversed(by_distance(lax.axis_size("row"))):
        remote(src_of(step), dst_of(step), send, recv_of(step), "row", step).start()


def exchange(src, dst, xs, xr):
    for d in range(1, lax.axis_size("col")):
        remote(
            src.at[place("col", d)], dst.at[lax.axis_index("col")], xs, xr.at[d], "col", d
        ).start()


def exchanged(dst, xs, xr):
    for d in range(1, lax.axis_size("col")):
        arrived(dst.at[place("col", -d)], xr.at[d])
    arrived(dst.at[pl.ds(0, lax.axis_size("col") - 1)], xs)


def over(a, b):
    return lax.dot_general(a, b, (((1,), (1,)), ((), ())), preferred_element_type=F32)


def under(a, b):
    return lax.dot_general(a, b, (((0,), (0,)), ((), ())), preferred_element_type=F32)


def plain(a, b):
    return lax.dot_general(a, b, (((1,), (0,)), ((), ())), preferred_element_type=F32)


def standardized(values):
    values = values.astype(F32)
    centred = values - jnp.mean(values, -1, keepdims=True)
    inverse = lax.rsqrt(jnp.mean(centred * centred, -1, keepdims=True) + EPSILON)
    return centred * inverse, inverse


def add_up(values):
    return functools.reduce(jnp.add, values)


def whole_kernel(
    scale, pair_far, cot_far, mask_far, w_qkvg_far, w_bias_far, w_out_far, update, grad, share_all,
    bias_all, pair, cot, mask, w_qkvg, w_bias, w_out, piece, bias, rows, cots, mask_own, masks,
    d_bias, bias_in, upd, upd_in, upd_other, dn, dn_in, dn_mine, dn_other, grads, grads_in, pieces,
    tiles, shares, shares_in, share_own, bias_own, bias_x, bias_row, ins, gzs, gzr, gxs, gxr, es,
    er, rs, rr, hs, hr, bs, br, ls, lr, cs, cr, ss, sr, fs, fr, fxs, fxr, ws, wr, vs, vr,
):
    length, width = lax.axis_size("row"), lax.axis_size("col")
    x, z = lax.axis_index("col"), lax.axis_index("row")
    _, row_count, block, channels = pair.shape
    cols = w_out.shape[0]
    size = cols // 2
    tokens, span = width * block, 2 * block
    full_rows = width * row_count
    steps = [("chan", 1)] + [("col", d) for d in range(1, width)]
    steps += [("row", s * t) for t in range(1, HOP + 1) for s in (1, -1)]
    barrier = pltpu.get_barrier_semaphore()
    for axis, step in steps:
        pl.semaphore_signal(
            barrier, inc=1, device_id={axis: place(axis, step)}, device_id_type=MESH
        )

    loads = [
        pltpu.make_async_copy(src, dst, ins.at[n])
        for n, (src, dst) in enumerate(
            (
                (pair_far, pair),
                (w_bias_far, w_bias),
                (mask_far, mask),
                (w_qkvg_far, w_qkvg),
                (cot_far, cot),
                (w_out_far, w_out),
            )
        )
    ]
    for load in loads:
        load.start()
    for load in loads[:2]:
        load.wait()
    standard, inverse = standardized(pair[...].reshape(full_rows * block, channels))
    normed_own = standard.astype(BF16)
    w_rows = w_bias[...].astype(F32)
    flat = over(w_bias[...], normed_own)
    lines = []
    for j in range(full_rows):
        part = flat[:, j * block : (j + 1) * block]
        lines += [jnp.concatenate([part[0:1], part[1:2]], 1)]
    piece[0] = jnp.concatenate(lines, 0)
    for load in loads[2:]:
        load.wait()
    valid = MASK_BIG * (mask[...].astype(F32) - 1.0)
    mask_own[...] = jnp.concatenate([valid, valid], 1)
    wqk = jnp.concatenate([w_qkvg[0], w_qkvg[1]], 0)
    wvg = jnp.concatenate([w_qkvg[2], w_qkvg[3]], 0)
    pl.semaphore_wait(barrier, len(steps))

    head_lane = lax.broadcasted_iota(jnp.int32, (block, cols), 1) < size
    lane = lax.broadcasted_iota(jnp.int32, (tokens, span), 1) < block
    lane_col = lax.broadcasted_iota(jnp.int32, (tokens, cols), 1) < size

    def doubled(values):
        parts = []
        for n in range(width):
            part = values[n * block : (n + 1) * block]
            zero = jnp.zeros_like(part)
            parts += [jnp.where(head_lane, part, zero), jnp.where(head_lane, zero, part)]
        return jnp.concatenate(parts, 0)

    def halved(values):
        parts = []
        for n in range(width):
            first = values[n * span : n * span + block]
            second = values[n * span + block : (n + 1) * span]
            parts += [jnp.where(head_lane, first, second)]
        return jnp.concatenate(parts, 0)

    def per_head(parts, joined, reduced, empty):
        both = functools.reduce(joined, parts)
        first = reduced(jnp.where(lane, both, empty), axis=1, keepdims=True)
        second = reduced(jnp.where(lane, empty, both), axis=1, keepdims=True)
        return jnp.where(lane, first, second)

    core = lax.axis_index("chan")
    halves = ((pair, rows), (cot, cots))
    known = []

    def start_exchange():
        for n, (src, dst) in enumerate(halves):
            for d in (2, 1, 3):
                half = src.at[place("col", d), core]
                remote(half, dst.at[x, core], rs.at[n, d], rr.at[n, d], "col", d).start()
        for d in (2, 1, 3):
            remote(mask_own, masks.at[x], es.at[2], er.at[2, d], "col", d).start()
        rows[x], cots[x], masks[x] = pair[x], cot[x], mask_own[...]

    def hand_over():
        for n, (src, dst) in enumerate(halves):
            for d in range(1, width):
                half = dst.at[place("col", -d), core]
                arrived(half, rr.at[n, d])
                remote(half, half, hs.at[n, d], hr.at[n, d], "chan", 1).start()
        for n, (src, dst) in enumerate(halves):
            for d in range(1, width):
                arrived(src.at[0, 0], rs.at[n, d])

    def project(r):
        normed = standardized(rows[:, r].reshape(tokens, channels))[0].astype(BF16)
        row_cot = cots[:, r].reshape(tokens, channels)
        qk, vg = over(normed, wqk), over(normed, wvg)
        query = (qk[:, :cols] * scale).astype(BF16)
        key2 = doubled(qk[:, cols:]).astype(BF16)
        value2 = doubled(vg[:, :cols]).astype(BF16)
        gate = jax.nn.sigmoid(vg[:, cols:])
        d_gated = over(row_cot, w_out[...])
        d_attended = (d_gated * gate).astype(BF16)
        scores = over(query, key2)
        d_weights = over(d_attended, value2)
        known.append(
            (normed, row_cot, query, key2, value2, gate, d_gated, d_attended, scores, d_weights)
        )

    def first_row():
        for n, (_, dst) in enumerate(halves):
            for d in range(1, width):
                arrived(dst.at[place("col", -d), 1 - core], hr.at[n, d])
                arrived(dst.at[0, 0], hs.at[n, d])
        exchanged(masks, es.at[2], er.at[2])
        project(0)

    def other_rows():
        for r in range(1, row_count):
            project(r)

    gaps = (start_exchange, hand_over, first_row, other_rows)
    gather_everywhere(piece, bias, gzs, gzr, gxs, gxr, gaps)
    blocks = [lax.rem(z + length - b, length) for b in range(length)]

    bias_sum = [None] * width
    saved = []
    for r in range(row_count):
        _, _, _, _, value2, _, _, d_attended, scores, d_weights = known[r]
        parts = [
            (scores[:, n * span : (n + 1) * span] + jnp.concatenate([bias[n, k] for k in blocks], 0))
            + masks[n, pl.ds(x * row_count + r, 1), :]
            for n in range(width)
        ]
        top = per_head(parts, jnp.maximum, jnp.max, -jnp.inf)
        parts = [jnp.exp(part - top) for part in parts]
        below = 1.0 / per_head(parts, jnp.add, jnp.sum, 0.0)
        weights = [part * below for part in parts]
        weights_b = jnp.concatenate([w.astype(BF16) for w in weights], 1)
        attended = plain(weights_b, value2)
        product = d_attended.astype(F32) * attended
        first = jnp.sum(jnp.where(lane_col, product, 0.0), axis=1, keepdims=True)
        second = jnp.sum(jnp.where(lane_col, 0.0, product), axis=1, keepdims=True)
        row_dot = jnp.where(lane, first, second)
        d_scores = [
            weights[n] * (d_weights[:, n * span : (n + 1) * span] - row_dot)
            for n in range(width)
        ]
        bias_sum = [d if b is None else b + d for b, d in zip(bias_sum, d_scores)]
        d_scores_b = jnp.concatenate([d.astype(BF16) for d in d_scores], 1)
        saved += [(weights_b, attended, d_scores_b)]
    for n in range(width):
        for b in range(length):
            part = bias_sum[n][b * full_rows : (b + 1) * full_rows]
            d_bias[n, lax.rem(b + length - z, length)] = part.astype(BF16)
    quarter, half = length // 4, length // 2
    step = quarter // 2
    groups = [((half - step, quarter),)]
    groups += [((half - n * step, step), (half + (n - 1) * step, step)) for n in range(2, 5)]

    def send_group(n):
        for first, count in groups[n]:
            slots = pl.ds(first, count)
            for d in (2, 1, 3):
                src = d_bias.at[place("col", d), slots]
                remote(src, bias_in.at[x, slots], bs, br.at[n, d], "col", d).start()

    send_group(0)
    bias_in[x] = d_bias[x]

    gqk = gvg = gout = None
    for r in range(row_count):
        normed, row_cot, query, key2, _, gate, d_gated, d_attended, _, _ = known[r]
        weights_b, attended, d_scores_b = saved[r]
        gated = (gate * attended).astype(BF16)
        upd[:, r] = plain(gated, w_out[...]).astype(BF16).reshape(width, block, channels)
        d_gate = d_gated * attended * gate * (1.0 - gate)
        d_query = plain(d_scores_b, key2) * scale
        d_key = halved(under(d_scores_b, query))
        d_value = halved(under(weights_b, d_attended))
        dqk = jnp.concatenate([d_query, d_key], 1).astype(BF16)
        dvg = jnp.concatenate([d_value, d_gate], 1).astype(BF16)
        back = plain(dqk, wqk) + plain(dvg, wvg)
        dn[:, r] = back.astype(BF16).reshape(width, block, channels)
        new = (under(dqk, normed), under(dvg, normed), under(gated, row_cot))
        if gqk is None:
            gqk, gvg, gout = new
        else:
            gqk, gvg, gout = gqk + new[0], gvg + new[1], gout + new[2]
    part_rows = grads.shape[1]
    everything = jnp.concatenate([gqk, gvg, gout], 0).astype(BF16)
    for n in range(width):
        grads[n] = everything[n * part_rows : (n + 1) * part_rows]
    sources = ((grads, grads_in), (upd, upd_in), (dn, dn_in))
    exchange(grads, grads_in, es.at[3], er.at[3])
    for n in range(1, 4):
        send_group(n)
    exchange(dn, dn_in, es.at[5], er.at[5])
    exchange(upd, upd_in, es.at[4], er.at[4])
    for src, dst in sources:
        dst[x] = src[x]

    def send_tiles(n):
        for d in range(1, width):
            arrived(bias_in.at[0, pl.ds(0, quarter)], br.at[n, d])
        slots = []
        for first, count in groups[n]:
            parts = [bias_in[m, first : first + count].astype(F32) for m in range(width)]
            pieces[first : first + count] = add_up(parts).astype(BF16)
            slots += range(first, first + count)
        for k in sorted(slots, key=lambda k: -min(k, length - k)):
            if k:
                remote(pieces.at[k], tiles.at[k], ls, lr, "row", k).start()

    send_tiles(0)
    exchanged(grads_in, es.at[3], er.at[3])
    summed = add_up([grads_in[n].astype(F32) for n in range(width)]).reshape(-1, HOP, channels)
    shares[...] = summed.astype(BF16)
    used = shares.shape[0]
    for step in reversed(by_distance(length)):
        dest = place("row", step)

        @pl.when(dest < used)
        def _():
            src = shares.at[dest]
            remote(src, shares_in.at[step % length], ss, sr, "row", step).start()

    for n in range(1, 4):
        send_tiles(n)
    tiles[0] = pieces[0]
    exchanged(dn_in, es.at[5], er.at[5])
    exchanged(upd_in, es.at[4], er.at[4])
    other = remote(upd_in, upd_other, cs.at[0], cr.at[0], "chan", 1)
    other.start()
    other.wait()
    update[...] = (upd_in[...].astype(F32) + upd_other[...].astype(F32)).astype(BF16)
    arrived(tiles.at[pl.ds(0, length - 1)], lr)
    tile = jnp.sum(tiles[...].astype(F32), 0)
    columns = jnp.transpose(tile)
    sums = [None, None]
    for j in range(full_rows):
        normed = normed_own[j * block : (j + 1) * block].astype(F32)
        for h in range(2):
            term = normed * columns[h * block : (h + 1) * block, j : j + 1]
            sums[h] = term if sums[h] is None else sums[h] + term
    sums = [jnp.sum(term, 0, keepdims=True) for term in sums]
    bias_own[...] = jnp.concatenate(sums, 0)
    for d in (2, 1, 3):
        remote(bias_own, bias_x.at[x], ws, wr.at[d], "col", d).start()
    bias_x[x] = bias_own[...]
    for j in range(full_rows):
        added = dn_in[j // row_count, j % row_count].astype(F32)
        for h in range(2):
            column = columns[h * block : (h + 1) * block, j : j + 1]
            added = added + column * w_rows[h : h + 1, :]
        dn_mine[j // row_count, j % row_count] = added.astype(BF16)
    other = remote(dn_mine, dn_other, cs.at[1], cr.at[1], "chan", 1)
    other.start()

    @pl.when(z < used)
    def _():
        shares_in[0] = shares[z]
        arrived(shares_in.at[pl.ds(0, length - 1)], sr)
        share_own[...] = jnp.sum(shares_in[...].astype(F32), 0).astype(BF16)
        slot = share_all.at[x, z]
        for step in reversed(by_distance(length)):
            remote(share_own, slot, fs, fr.at[step % length], "row", step).start()
        for d in (2, 1, 3):
            remote(share_own, slot, fxs, fxr.at[d], "col", d).start()
        share_all[x, z] = share_own[...]

    exchanged(bias_x, ws, wr)
    bias_row[...] = jnp.sum(bias_x[...], 0)
    to_all_rows(
        lambda step: bias_row, lambda step: bias_all.at[step % length], vs, lambda step: vr
    )
    bias_all[0] = bias_row[...]

    other.wait()
    d_total = dn_mine[...].astype(F32) + dn_other[...].astype(F32)
    d_total = d_total.reshape(full_rows * block, channels)
    centred = d_total - jnp.mean(d_total, -1, keepdims=True)
    centred = centred - standard * jnp.mean(d_total * standard, -1, keepdims=True)
    grad[...] = (inverse * centred).astype(BF16).reshape(grad.shape)

    for step in by_distance(length):
        source = place("row", -step)

        @pl.when(source < used)
        def _():
            slot = share_all.at[x, source]
            arrived(slot, fr.at[step % length])
            for d in (2, 1, 3):
                remote(slot, slot, fxs, fxr.at[d], "col", d).start()

    arrived(bias_all.at[pl.ds(0, length - 1)], vr)
    for d in range(1, width):
        arrived(share_all.at[place("col", -d)], fxr.at[d])
    arrived(bias_all.at[pl.ds(0, length - 1)], vs)

    @pl.when(z < used)
    def _():
        arrived(shares_in.at[pl.ds(0, length - 1)], fs)
        arrived(shares.at[pl.ds(0, used - 1)], ss)

    @pl.when(z >= used)
    def _():
        arrived(shares, ss)

    arrived(share_all.at[pl.ds(0, width - 1)], fxs)
    arrived(bias_in.at[pl.ds(0, width - 1)], bs)
    arrived(pieces.at[pl.ds(0, length - 1)], ls)


def finish_kernel(tokens, update_in, grad_in, share_all, bias_all, update, grad, qkvg, bias, out):
    update[...] = update_in[...]
    grad[...] = grad_in[...]
    _, cols, channels = qkvg.shape
    total = 4 * cols + out.shape[0]
    rows = share_all[...].astype(F32).reshape(total, channels) / tokens
    qkvg[...] = rows[: 4 * cols].reshape(qkvg.shape)
    out[...] = rows[4 * cols :]
    bias[...] = jnp.sum(bias_all[...], 0) / tokens


def call(kernel, name, identity, outs, scratch, *args, near=pltpu.VMEM):
    params = dict(vmem_limit_bytes=24 * 2**20)
    if identity is not None:
        params.update(collective_id=identity, has_side_effects=True)
    vmem = pl.BlockSpec(memory_space=pltpu.VMEM)
    return pl.pallas_call(
        kernel,
        out_shape=[jax.ShapeDtypeStruct(shape, kind) for shape, kind in outs],
        in_specs=[pl.BlockSpec(memory_space=near)] * len(args),
        out_specs=[vmem] * len(outs),
        scratch_shapes=scratch,
        compiler_params=pltpu.CompilerParams(**params),
        name=name,
    )(*args)


def on_device(pair_rep, pair_mask, w_qkvg, w_bias, w_out, cotangent):
    full_rows, block, channels = pair_rep.shape
    length, width = lax.axis_size("row"), lax.axis_size("col")
    cols = w_qkvg.shape[2]
    heads = w_bias.shape[1]
    scale = (cols // heads) ** (-0.5)
    tokens = width * block
    span = heads * block
    tiled = (width, full_rows // width, block, channels)
    part = (2 * channels + cols) // width
    message = (full_rows, span)
    V = pltpu.VMEM
    gathered = (width, length) + message
    share = (HOP, channels)
    tile = V(tiled, BF16)
    stored = jnp.transpose(w_qkvg, (0, 2, 1))
    args = (
        pair_rep.reshape(tiled),
        cotangent.reshape(tiled),
        pair_mask,
        stored,
        w_bias.T,
        w_out,
    )
    scratch = [V(arg.shape, arg.dtype) for arg in args]
    scratch += [V((1,) + message, F32), V(gathered, F32), tile, tile]
    scratch += [V(message, F32), V((width,) + message, F32)]
    scratch += [V(gathered, BF16)] * 2 + [tile] * 7
    scratch += [V((width, part, channels), BF16)] * 2 + [V((length,) + message, BF16)] * 2
    scratch += [V((part // HOP,) + share, BF16), V((length,) + share, BF16), V(share, BF16)]
    scratch += [V((heads, channels), F32), V((width, heads, channels), F32)]
    scratch += [V((heads, channels), F32)]
    scratch += [DMA((len(args),)), DMA, DMA((length,)), DMA, DMA((width,))]
    scratch += [DMA((6,)), DMA((6, width))] + [DMA((2, width))] * 4 + [DMA, DMA((4, width))]
    scratch += [DMA, DMA, DMA((2,)), DMA((2,))]
    scratch += [DMA, DMA, DMA, DMA((length,)), DMA, DMA((width,))]
    scratch += [DMA, DMA((width,)), DMA, DMA]
    update, grad, share_all, bias_all = call(
        functools.partial(whole_kernel, scale),
        "whole",
        0,
        [
            (tiled, BF16),
            (tiled, BF16),
            ((width, part // HOP) + share, BF16),
            ((length, heads, channels), F32),
        ],
        scratch,
        *(pltpu.with_memory_space_constraint(arg, pltpu.HBM) for arg in args),
        near=pltpu.HBM,
    )
    shape = pair_rep.shape
    update, grad, qkvg, bias_grad, out = call(
        functools.partial(finish_kernel, tokens),
        "finish",
        None,
        [
            (tiled, BF16),
            (tiled, BF16),
            (stored.shape, F32),
            (w_bias.T.shape, F32),
            (w_out.shape, F32),
        ],
        [],
        update,
        grad,
        share_all,
        bias_all,
    )
    qkvg = jnp.transpose(qkvg, (0, 2, 1))
    return (update.reshape(shape), grad.reshape(shape), qkvg, bias_grad.T, out)


def solution(mesh):
    in_specs = (
        P(("groups", "row"), "col", None),
        P(("groups", "row"), "col"),
        P(None, None, "chan"),
        P(None, "chan"),
        P("chan", None),
        P(("groups", "row"), "col", None),
    )
    out_specs = (
        P(("groups", "row"), "col", None),
        P(("groups", "row"), "col", None),
        P("groups", None, "chan"),
        P("groups", "chan"),
        P("chan", "groups"),
    )
    return jax.shard_map(
        on_device, mesh=mesh, in_specs=in_specs, out_specs=out_specs, check_vma=False
    )
```

```python
import functools

import jax
import jax.numpy as jnp
from jax import lax
from jax.experimental import pallas as pl
from jax.experimental.pallas import tpu as pltpu
from jax.sharding import PartitionSpec as P

EPSILON = 1e-05
MASK_BIG = 1000000000.0
MESH = pl.DeviceIdType.MESH
F32 = jnp.float32
BF16 = jnp.bfloat16
HOP = 4
DMA = pltpu.SemaphoreType.DMA


def place(axis, step):
    size = lax.axis_size(axis)
    return lax.rem(lax.axis_index(axis) + (step % size), size)


def remote(src, dst, send, recv, axis, step):
    return pltpu.make_async_remote_copy(
        src_ref=src,
        dst_ref=dst,
        send_sem=send,
        recv_sem=recv,
        device_id={axis: place(axis, step)},
        device_id_type=MESH,
    )


def arrived(dst, recv):
    pltpu.make_async_copy(dst, dst, recv).wait()


def gather_everywhere(piece, out, zs, zr, xs, xr, gaps):
    length, width = lax.axis_size("row"), lax.axis_size("col")
    x, half = lax.axis_index("col"), length // 2
    last = half // HOP

    def along_row(src, delta, steps):
        for step in steps:
            k = (delta + step) % length
            remote(src, out.at[x, k], zs, zr.at[k], "row", step).start()

    def along_col(src, first, count):
        slots = out.at[x, pl.ds(first, count)]
        for d in (2, 1, 3):
            remote(slots if src is None else src, slots, xs, xr.at[d], "col", d).start()

    def wait(delta):
        arrived(out.at[x, delta % length], zr.at[delta % length])

    along_row(piece.at[0], 0, [s * t for t in (HOP, 3, 2, 1) for s in (1, -1)])
    along_col(piece, 0, 1)
    out[x, 0] = piece[0]
    gaps[0]()
    for a in range(1, last):
        for s in (1, -1):
            wait(s * HOP * a)
            far = [s * HOP] if (s == 1 or a < last - 1) else []
            along_row(out.at[x, s * HOP * a % length], s * HOP * a, far + [s * t for t in (3, 2, 1)])
        for s in (1, -1):
            for t in range(1, HOP):
                wait(s * (HOP * (a - 1) + t))
            along_col(None, HOP * (a - 1) + 1 if s == 1 else length - HOP * a, HOP)
        gaps[a]()
    for t in range(1, HOP):
        for s in (1, -1):
            wait(s * (half - HOP + t))
    along_col(None, half + 1, HOP - 1)
    along_col(None, half - HOP + 1, HOP - 1)
    wait(half)
    along_col(None, half, 1)
    for d in range(1, width):
        arrived(out.at[place("col", -d)], xr.at[d])
    arrived(out.at[0, pl.ds(0, length - 1)], zs)
    arrived(out.at[pl.ds(0, width - 1)], xs)


def by_distance(length):
    return [s * t for t in range(1, length // 2) for s in (1, -1)] + [length // 2]


def to_all_rows(src_of, dst_of, send, recv_of):
    for step in reversed(by_distance(lax.axis_size("row"))):
        remote(src_of(step), dst_of(step), send, recv_of(step), "row", step).start()


def exchange(src, dst, xs, xr):
    for d in range(1, lax.axis_size("col")):
        remote(
            src.at[place("col", d)], dst.at[lax.axis_index("col")], xs, xr.at[d], "col", d
        ).start()


def exchanged(dst, xs, xr):
    for d in range(1, lax.axis_size("col")):
        arrived(dst.at[place("col", -d)], xr.at[d])
    arrived(dst.at[pl.ds(0, lax.axis_size("col") - 1)], xs)


def over(a, b):
    return lax.dot_general(a, b, (((1,), (1,)), ((), ())), preferred_element_type=F32)


def under(a, b):
    return lax.dot_general(a, b, (((0,), (0,)), ((), ())), preferred_element_type=F32)


def plain(a, b):
    return lax.dot_general(a, b, (((1,), (0,)), ((), ())), preferred_element_type=F32)


def standardized(values):
    values = values.astype(F32)
    centred = values - jnp.mean(values, -1, keepdims=True)
    inverse = lax.rsqrt(jnp.mean(centred * centred, -1, keepdims=True) + EPSILON)
    return centred * inverse, inverse


def add_up(values):
    return functools.reduce(jnp.add, values)


def whole_kernel(
    scale, pair_far, cot_far, mask_far, w_qkvg_far, w_bias_far, w_out_far, update, grad, share_all,
    bias_all, pair, cot, mask, w_qkvg, w_bias, w_out, piece, bias, rows, cots, mask_own, masks,
    d_bias, bias_in, upd, upd_in, upd_other, dn, dn_in, dn_mine, dn_other, grads, grads_in, pieces,
    tiles, shares, shares_in, share_own, bias_own, bias_x, bias_row, ins, gzs, gzr, gxs, gxr, es,
    er, entered, bs, br, ls, lr, cs, cr, ss, sr, fs, fr, fxs, fxr, ws, wr, vs, vr,
):
    length, width = lax.axis_size("row"), lax.axis_size("col")
    x, z = lax.axis_index("col"), lax.axis_index("row")
    _, row_count, block, channels = pair.shape
    cols = w_out.shape[0]
    size = cols // 2
    tokens, span = width * block, 2 * block
    full_rows = width * row_count
    steps = [("col", d) for d in range(1, width)]
    steps += [("row", s * t) for t in range(1, HOP + 1) for s in (1, -1)]
    barrier = pltpu.get_barrier_semaphore()
    for axis, step in steps:
        pl.semaphore_signal(
            barrier, inc=1, device_id={axis: place(axis, step)}, device_id_type=MESH
        )

    core = lax.axis_index("chan")

    @pl.when(core == 0)
    def _():
        pl.semaphore_signal(
            barrier, inc=1, device_id={"chan": place("chan", 1)}, device_id_type=MESH
        )

    loads = [
        pltpu.make_async_copy(src, dst, ins.at[n])
        for n, (src, dst) in enumerate(
            (
                (pair_far, pair),
                (w_bias_far, w_bias),
                (mask_far, mask),
                (w_qkvg_far, w_qkvg),
                (cot_far, cot),
                (w_out_far, w_out),
            )
        )
    ]
    for load in loads:
        load.start()
    for load in loads[:2]:
        load.wait()
    standard, inverse = standardized(pair[...].reshape(full_rows * block, channels))
    normed_own = standard.astype(BF16)
    w_rows = w_bias[...].astype(F32)
    flat = over(w_bias[...], normed_own)
    lines = []
    for j in range(full_rows):
        part = flat[:, j * block : (j + 1) * block]
        lines += [jnp.concatenate([part[0:1], part[1:2]], 1)]
    piece[0] = jnp.concatenate(lines, 0)
    for load in loads[2:]:
        load.wait()
    valid = MASK_BIG * (mask[...].astype(F32) - 1.0)
    mask_own[...] = jnp.concatenate([valid, valid], 1)
    wqk = jnp.concatenate([w_qkvg[0], w_qkvg[1]], 0)
    wvg = jnp.concatenate([w_qkvg[2], w_qkvg[3]], 0)
    pl.semaphore_wait(barrier, len(steps) + core)

    @pl.when(core == 1)
    def _():
        pl.semaphore_signal(
            entered, inc=1, device_id={"chan": place("chan", 1)}, device_id_type=MESH
        )


    head_lane = lax.broadcasted_iota(jnp.int32, (block, cols), 1) < size
    lane = lax.broadcasted_iota(jnp.int32, (tokens, span), 1) < block
    lane_col = lax.broadcasted_iota(jnp.int32, (tokens, cols), 1) < size

    def doubled(values):
        parts = []
        for n in range(width):
            part = values[n * block : (n + 1) * block]
            zero = jnp.zeros_like(part)
            parts += [jnp.where(head_lane, part, zero), jnp.where(head_lane, zero, part)]
        return jnp.concatenate(parts, 0)

    def halved(values):
        parts = []
        for n in range(width):
            first = values[n * span : n * span + block]
            second = values[n * span + block : (n + 1) * span]
            parts += [jnp.where(head_lane, first, second)]
        return jnp.concatenate(parts, 0)

    def per_head(parts, joined, reduced, empty):
        both = functools.reduce(joined, parts)
        first = reduced(jnp.where(lane, both, empty), axis=1, keepdims=True)
        second = reduced(jnp.where(lane, empty, both), axis=1, keepdims=True)
        return jnp.where(lane, first, second)

    known = []

    def start_exchange():
        exchange(pair, rows, es.at[0], er.at[0])
        exchange(cot, cots, es.at[1], er.at[1])
        for d in range(1, width):
            remote(mask_own, masks.at[x], es.at[2], er.at[2, d], "col", d).start()
        rows[x], cots[x], masks[x] = pair[x], cot[x], mask_own[...]

    def project(r):
        normed = standardized(rows[:, r].reshape(tokens, channels))[0].astype(BF16)
        row_cot = cots[:, r].reshape(tokens, channels)
        qk, vg = over(normed, wqk), over(normed, wvg)
        query = (qk[:, :cols] * scale).astype(BF16)
        key2 = doubled(qk[:, cols:]).astype(BF16)
        value2 = doubled(vg[:, :cols]).astype(BF16)
        gate = jax.nn.sigmoid(vg[:, cols:])
        d_gated = over(row_cot, w_out[...])
        d_attended = (d_gated * gate).astype(BF16)
        scores = over(query, key2)
        d_weights = over(d_attended, value2)
        known.append(
            (normed, row_cot, query, key2, value2, gate, d_gated, d_attended, scores, d_weights)
        )

    def first_row():
        for n, dst in enumerate((rows, cots, masks)):
            exchanged(dst, es.at[n], er.at[n])
        project(0)

    def other_rows():
        for r in range(1, row_count):
            project(r)

    gaps = (start_exchange, lambda: None, first_row, other_rows)
    gather_everywhere(piece, bias, gzs, gzr, gxs, gxr, gaps)
    blocks = [lax.rem(z + length - b, length) for b in range(length)]

    bias_sum = [None] * width
    saved = []
    for r in range(row_count):
        _, _, _, _, value2, _, _, d_attended, scores, d_weights = known[r]
        parts = [
            (scores[:, n * span : (n + 1) * span] + jnp.concatenate([bias[n, k] for k in blocks], 0))
            + masks[n, pl.ds(x * row_count + r, 1), :]
            for n in range(width)
        ]
        top = per_head(parts, jnp.maximum, jnp.max, -jnp.inf)
        parts = [jnp.exp(part - top) for part in parts]
        below = 1.0 / per_head(parts, jnp.add, jnp.sum, 0.0)
        weights = [part * below for part in parts]
        weights_b = jnp.concatenate([w.astype(BF16) for w in weights], 1)
        attended = plain(weights_b, value2)
        product = d_attended.astype(F32) * attended
        first = jnp.sum(jnp.where(lane_col, product, 0.0), axis=1, keepdims=True)
        second = jnp.sum(jnp.where(lane_col, 0.0, product), axis=1, keepdims=True)
        row_dot = jnp.where(lane, first, second)
        d_scores = [
            weights[n] * (d_weights[:, n * span : (n + 1) * span] - row_dot)
            for n in range(width)
        ]
        bias_sum = [d if b is None else b + d for b, d in zip(bias_sum, d_scores)]
        d_scores_b = jnp.concatenate([d.astype(BF16) for d in d_scores], 1)
        saved += [(weights_b, attended, d_scores_b)]
    for n in range(width):
        for b in range(length):
            part = bias_sum[n][b * full_rows : (b + 1) * full_rows]
            d_bias[n, lax.rem(b + length - z, length)] = part.astype(BF16)
    quarter, half = length // 4, length // 2
    step = quarter // 2
    groups = [((half - step, quarter),)]
    groups += [((half - n * step, step), (half + (n - 1) * step, step)) for n in range(2, 5)]

    def send_group(n):
        for first, count in groups[n]:
            slots = pl.ds(first, count)
            for d in (2, 1, 3):
                src = d_bias.at[place("col", d), slots]
                remote(src, bias_in.at[x, slots], bs, br.at[n, d], "col", d).start()

    send_group(0)
    bias_in[x] = d_bias[x]

    gqk = gvg = gout = None
    for r in range(row_count):
        normed, row_cot, query, key2, _, gate, d_gated, d_attended, _, _ = known[r]
        weights_b, attended, d_scores_b = saved[r]
        gated = (gate * attended).astype(BF16)
        upd[:, r] = plain(gated, w_out[...]).astype(BF16).reshape(width, block, channels)
        d_gate = d_gated * attended * gate * (1.0 - gate)
        d_query = plain(d_scores_b, key2) * scale
        d_key = halved(under(d_scores_b, query))
        d_value = halved(under(weights_b, d_attended))
        dqk = jnp.concatenate([d_query, d_key], 1).astype(BF16)
        dvg = jnp.concatenate([d_value, d_gate], 1).astype(BF16)
        back = plain(dqk, wqk) + plain(dvg, wvg)
        dn[:, r] = back.astype(BF16).reshape(width, block, channels)
        new = (under(dqk, normed), under(dvg, normed), under(gated, row_cot))
        if gqk is None:
            gqk, gvg, gout = new
        else:
            gqk, gvg, gout = gqk + new[0], gvg + new[1], gout + new[2]
    part_rows = grads.shape[1]
    everything = jnp.concatenate([gqk, gvg, gout], 0).astype(BF16)
    for n in range(width):
        grads[n] = everything[n * part_rows : (n + 1) * part_rows]
    sources = ((grads, grads_in), (upd, upd_in), (dn, dn_in))
    exchange(grads, grads_in, es.at[3], er.at[3])
    for n in range(1, 4):
        send_group(n)
    exchange(dn, dn_in, es.at[5], er.at[5])
    exchange(upd, upd_in, es.at[4], er.at[4])
    for src, dst in sources:
        dst[x] = src[x]

    def send_tiles(n):
        for d in range(1, width):
            arrived(bias_in.at[0, pl.ds(0, quarter)], br.at[n, d])
        slots = []
        for first, count in groups[n]:
            parts = [bias_in[m, first : first + count].astype(F32) for m in range(width)]
            pieces[first : first + count] = add_up(parts).astype(BF16)
            slots += range(first, first + count)
        for k in sorted(slots, key=lambda k: -min(k, length - k)):
            if k:
                remote(pieces.at[k], tiles.at[k], ls, lr, "row", k).start()

    send_tiles(0)
    exchanged(grads_in, es.at[3], er.at[3])
    summed = add_up([grads_in[n].astype(F32) for n in range(width)]).reshape(-1, HOP, channels)
    shares[...] = summed.astype(BF16)
    used = shares.shape[0]
    for step in reversed(by_distance(length)):
        dest = place("row", step)

        @pl.when(dest < used)
        def _():
            src = shares.at[dest]
            remote(src, shares_in.at[step % length], ss, sr, "row", step).start()

    for n in range(1, 4):
        send_tiles(n)
    tiles[0] = pieces[0]
    exchanged(dn_in, es.at[5], er.at[5])
    exchanged(upd_in, es.at[4], er.at[4])

    @pl.when(core == 0)
    def _():
        pl.semaphore_wait(entered, 1)

    other = remote(upd_in, upd_other, cs.at[0], cr.at[0], "chan", 1)
    other.start()
    other.wait()
    update[...] = (upd_in[...].astype(F32) + upd_other[...].astype(F32)).astype(BF16)
    arrived(tiles.at[pl.ds(0, length - 1)], lr)
    tile = jnp.sum(tiles[...].astype(F32), 0)
    columns = jnp.transpose(tile)
    sums = [None, None]
    for j in range(full_rows):
        normed = normed_own[j * block : (j + 1) * block].astype(F32)
        for h in range(2):
            term = normed * columns[h * block : (h + 1) * block, j : j + 1]
            sums[h] = term if sums[h] is None else sums[h] + term
    sums = [jnp.sum(term, 0, keepdims=True) for term in sums]
    bias_own[...] = jnp.concatenate(sums, 0)
    for d in (2, 1, 3):
        remote(bias_own, bias_x.at[x], ws, wr.at[d], "col", d).start()
    bias_x[x] = bias_own[...]
    for j in range(full_rows):
        added = dn_in[j // row_count, j % row_count].astype(F32)
        for h in range(2):
            column = columns[h * block : (h + 1) * block, j : j + 1]
            added = added + column * w_rows[h : h + 1, :]
        dn_mine[j // row_count, j % row_count] = added.astype(BF16)
    other = remote(dn_mine, dn_other, cs.at[1], cr.at[1], "chan", 1)
    other.start()

    @pl.when(z < used)
    def _():
        shares_in[0] = shares[z]
        arrived(shares_in.at[pl.ds(0, length - 1)], sr)
        share_own[...] = jnp.sum(shares_in[...].astype(F32), 0).astype(BF16)
        slot = share_all.at[x, z]
        for step in reversed(by_distance(length)):
            remote(share_own, slot, fs, fr.at[step % length], "row", step).start()
        for d in (2, 1, 3):
            remote(share_own, slot, fxs, fxr.at[d], "col", d).start()
        share_all[x, z] = share_own[...]

    exchanged(bias_x, ws, wr)
    bias_row[...] = jnp.sum(bias_x[...], 0)
    to_all_rows(
        lambda step: bias_row, lambda step: bias_all.at[step % length], vs, lambda step: vr
    )
    bias_all[0] = bias_row[...]

    other.wait()
    d_total = dn_mine[...].astype(F32) + dn_other[...].astype(F32)
    d_total = d_total.reshape(full_rows * block, channels)
    centred = d_total - jnp.mean(d_total, -1, keepdims=True)
    centred = centred - standard * jnp.mean(d_total * standard, -1, keepdims=True)
    grad[...] = (inverse * centred).astype(BF16).reshape(grad.shape)

    for step in by_distance(length):
        source = place("row", -step)

        @pl.when(source < used)
        def _():
            slot = share_all.at[x, source]
            arrived(slot, fr.at[step % length])
            for d in (2, 1, 3):
                remote(slot, slot, fxs, fxr.at[d], "col", d).start()

    arrived(bias_all.at[pl.ds(0, length - 1)], vr)
    for d in range(1, width):
        arrived(share_all.at[place("col", -d)], fxr.at[d])
    arrived(bias_all.at[pl.ds(0, length - 1)], vs)

    @pl.when(z < used)
    def _():
        arrived(shares_in.at[pl.ds(0, length - 1)], fs)
        arrived(shares.at[pl.ds(0, used - 1)], ss)

    @pl.when(z >= used)
    def _():
        arrived(shares, ss)

    arrived(share_all.at[pl.ds(0, width - 1)], fxs)
    arrived(bias_in.at[pl.ds(0, width - 1)], bs)
    arrived(pieces.at[pl.ds(0, length - 1)], ls)


def finish_kernel(tokens, update_in, grad_in, share_all, bias_all, update, grad, qkvg, bias, out):
    update[...] = update_in[...]
    grad[...] = grad_in[...]
    _, cols, channels = qkvg.shape
    total = 4 * cols + out.shape[0]
    rows = share_all[...].astype(F32).reshape(total, channels) / tokens
    qkvg[...] = rows[: 4 * cols].reshape(qkvg.shape)
    out[...] = rows[4 * cols :]
    bias[...] = jnp.sum(bias_all[...], 0) / tokens


def call(kernel, name, identity, outs, scratch, *args, near=pltpu.VMEM):
    params = dict(vmem_limit_bytes=24 * 2**20)
    if identity is not None:
        params.update(collective_id=identity, has_side_effects=True)
    vmem = pl.BlockSpec(memory_space=pltpu.VMEM)
    return pl.pallas_call(
        kernel,
        out_shape=[jax.ShapeDtypeStruct(shape, kind) for shape, kind in outs],
        in_specs=[pl.BlockSpec(memory_space=near)] * len(args),
        out_specs=[vmem] * len(outs),
        scratch_shapes=scratch,
        compiler_params=pltpu.CompilerParams(**params),
        name=name,
    )(*args)


def on_device(pair_rep, pair_mask, w_qkvg, w_bias, w_out, cotangent):
    full_rows, block, channels = pair_rep.shape
    length, width = lax.axis_size("row"), lax.axis_size("col")
    cols = w_qkvg.shape[2]
    heads = w_bias.shape[1]
    scale = (cols // heads) ** (-0.5)
    tokens = width * block
    span = heads * block
    tiled = (width, full_rows // width, block, channels)
    part = (2 * channels + cols) // width
    message = (full_rows, span)
    V = pltpu.VMEM
    gathered = (width, length) + message
    share = (HOP, channels)
    tile = V(tiled, BF16)
    stored = jnp.transpose(w_qkvg, (0, 2, 1))
    args = (
        pair_rep.reshape(tiled),
        cotangent.reshape(tiled),
        pair_mask,
        stored,
        w_bias.T,
        w_out,
    )
    scratch = [V(arg.shape, arg.dtype) for arg in args]
    scratch += [V((1,) + message, F32), V(gathered, F32), tile, tile]
    scratch += [V(message, F32), V((width,) + message, F32)]
    scratch += [V(gathered, BF16)] * 2 + [tile] * 7
    scratch += [V((width, part, channels), BF16)] * 2 + [V((length,) + message, BF16)] * 2
    scratch += [V((part // HOP,) + share, BF16), V((length,) + share, BF16), V(share, BF16)]
    scratch += [V((heads, channels), F32), V((width, heads, channels), F32)]
    scratch += [V((heads, channels), F32)]
    scratch += [DMA((len(args),)), DMA, DMA((length,)), DMA, DMA((width,))]
    scratch += [DMA((6,)), DMA((6, width)), pltpu.SemaphoreType.REGULAR, DMA, DMA((4, width))]
    scratch += [DMA, DMA, DMA((2,)), DMA((2,))]
    scratch += [DMA, DMA, DMA, DMA((length,)), DMA, DMA((width,))]
    scratch += [DMA, DMA((width,)), DMA, DMA]
    update, grad, share_all, bias_all = call(
        functools.partial(whole_kernel, scale),
        "whole",
        0,
        [
            (tiled, BF16),
            (tiled, BF16),
            ((width, part // HOP) + share, BF16),
            ((length, heads, channels), F32),
        ],
        scratch,
        *(pltpu.with_memory_space_constraint(arg, pltpu.HBM) for arg in args),
        near=pltpu.HBM,
    )
    shape = pair_rep.shape
    update, grad, qkvg, bias_grad, out = call(
        functools.partial(finish_kernel, tokens),
        "finish",
        None,
        [
            (tiled, BF16),
            (tiled, BF16),
            (stored.shape, F32),
            (w_bias.T.shape, F32),
            (w_out.shape, F32),
        ],
        [],
        update,
        grad,
        share_all,
        bias_all,
    )
    qkvg = jnp.transpose(qkvg, (0, 2, 1))
    return (update.reshape(shape), grad.reshape(shape), qkvg, bias_grad.T, out)


def solution(mesh):
    in_specs = (
        P(("groups", "row"), "col", None),
        P(("groups", "row"), "col"),
        P(None, None, "chan"),
        P(None, "chan"),
        P("chan", None),
        P(("groups", "row"), "col", None),
    )
    out_specs = (
        P(("groups", "row"), "col", None),
        P(("groups", "row"), "col", None),
        P("groups", None, "chan"),
        P("groups", "chan"),
        P("chan", "groups"),
    )
    return jax.shard_map(
        on_device, mesh=mesh, in_specs=in_specs, out_specs=out_specs, check_vma=False
    )
```

```python
import functools

import jax
import jax.numpy as jnp
from jax import lax
from jax.experimental import pallas as pl
from jax.experimental.pallas import tpu as pltpu
from jax.sharding import PartitionSpec as P

EPSILON = 1e-05
MASK_BIG = 1000000000.0
MESH = pl.DeviceIdType.MESH
F32 = jnp.float32
BF16 = jnp.bfloat16
HOP = 4
DMA = pltpu.SemaphoreType.DMA


def place(axis, step):
    size = lax.axis_size(axis)
    return lax.rem(lax.axis_index(axis) + (step % size), size)


def remote(src, dst, send, recv, axis, step):
    return pltpu.make_async_remote_copy(
        src_ref=src,
        dst_ref=dst,
        send_sem=send,
        recv_sem=recv,
        device_id={axis: place(axis, step)},
        device_id_type=MESH,
    )


def arrived(dst, recv):
    pltpu.make_async_copy(dst, dst, recv).wait()


def gather_everywhere(piece, out, zs, zr, xs, xr, hs, hr, gaps):
    length, width = lax.axis_size("row"), lax.axis_size("col")
    x, half = lax.axis_index("col"), length // 2
    last = half // HOP
    core = lax.axis_index("chan")

    def along_row(src, delta, steps):
        for step in steps:
            k = (delta + step) % length
            remote(src, out.at[x, k], zs, zr.at[k], "row", step).start()

    def along_col(src, first, count):
        slots = out.at[x, pl.ds(first, count)]
        for d in (2, 1, 3):
            remote(slots if src is None else src, slots, xs, xr.at[d], "col", d).start()

    def wait(delta):
        arrived(out.at[x, delta % length], zr.at[delta % length])

    @pl.when(core == 0)
    def _():
        remote(piece.at[0, 0], piece.at[0, 0], hs.at[0], hr.at[0], "chan", 1).start()

    @pl.when(core == 1)
    def _():
        arrived(piece.at[0, 0], hr.at[0])
        along_row(piece.at[0], 0, [s * t for t in (HOP, 3, 2, 1) for s in (1, -1)])
        along_col(piece, 0, 1)
        out[x, 0] = piece[0]

    gaps[0]()
    for a in range(1, last):

        @pl.when(core == 1)
        def _():
            for s in (1, -1):
                delta = s * HOP * a
                wait(delta)
                far = [s * HOP] if (s == 1 or a < last - 1) else []
                along_row(out.at[x, delta % length], delta, far + [s * t for t in (3, 2, 1)])
            for s in (1, -1):
                for t in range(1, HOP):
                    wait(s * (HOP * (a - 1) + t))
                along_col(None, HOP * (a - 1) + 1 if s == 1 else length - HOP * a, HOP)

        gaps[a]()

    @pl.when(core == 1)
    def _():
        for t in range(1, HOP):
            for s in (1, -1):
                wait(s * (half - HOP + t))
        along_col(None, half + 1, HOP - 1)
        along_col(None, half - HOP + 1, HOP - 1)
        wait(half)
        along_col(None, half, 1)
        for d in range(width):
            column = place("col", -d)
            if d:
                arrived(out.at[column], xr.at[d])
            slab = out.at[column, pl.ds(0, length), 0]
            remote(slab, slab, hs.at[1 + d], hr.at[1 + d], "chan", 1).start()
        arrived(out.at[0, pl.ds(0, length - 1)], zs)
        arrived(out.at[pl.ds(0, width - 1)], xs)
        for d in range(width):
            arrived(out.at[0, pl.ds(0, half)], hs.at[1 + d])

    @pl.when(core == 0)
    def _():
        for d in range(width):
            arrived(out.at[0, pl.ds(0, half)], hr.at[1 + d])
        arrived(piece.at[0, 0], hs.at[0])


def by_distance(length):
    return [s * t for t in range(1, length // 2) for s in (1, -1)] + [length // 2]


def to_all_rows(src_of, dst_of, send, recv_of):
    for step in reversed(by_distance(lax.axis_size("row"))):
        remote(src_of(step), dst_of(step), send, recv_of(step), "row", step).start()


def exchange(src, dst, xs, xr):
    for d in range(1, lax.axis_size("col")):
        remote(
            src.at[place("col", d)], dst.at[lax.axis_index("col")], xs, xr.at[d], "col", d
        ).start()


def exchanged(dst, xs, xr):
    for d in range(1, lax.axis_size("col")):
        arrived(dst.at[place("col", -d)], xr.at[d])
    arrived(dst.at[pl.ds(0, lax.axis_size("col") - 1)], xs)


def over(a, b):
    return lax.dot_general(a, b, (((1,), (1,)), ((), ())), preferred_element_type=F32)


def under(a, b):
    return lax.dot_general(a, b, (((0,), (0,)), ((), ())), preferred_element_type=F32)


def plain(a, b):
    return lax.dot_general(a, b, (((1,), (0,)), ((), ())), preferred_element_type=F32)


def standardized(values):
    values = values.astype(F32)
    centred = values - jnp.mean(values, -1, keepdims=True)
    inverse = lax.rsqrt(jnp.mean(centred * centred, -1, keepdims=True) + EPSILON)
    return centred * inverse, inverse


def add_up(values):
    return functools.reduce(jnp.add, values)


def whole_kernel(
    scale, pair_far, cot_far, mask_far, w_qkvg_far, w_bias_far, w_out_far, update, grad, share_all,
    bias_all, pair, cot, mask, w_qkvg, w_bias, w_out, piece, bias, rows, cots, mask_own, masks,
    d_bias, bias_in, upd, upd_in, upd_other, dn, dn_in, dn_mine, dn_other, grads, grads_in, pieces,
    tiles, shares, shares_in, share_own, bias_own, bias_x, bias_row, ins, gzs, gzr, gxs, gxr, es,
    er, rs, rr, hs, hr, gs, gr, bs, br, ls, lr, cs, cr, ss, sr, fs, fr, fxs, fxr, ws, wr, vs, vr,
):
    length, width = lax.axis_size("row"), lax.axis_size("col")
    x, z = lax.axis_index("col"), lax.axis_index("row")
    _, row_count, block, channels = pair.shape
    cols = w_out.shape[0]
    size = cols // 2
    tokens, span = width * block, 2 * block
    full_rows = width * row_count
    steps = [("chan", 1)] + [("col", d) for d in range(1, width)]
    steps += [("row", s * t) for t in range(1, HOP + 1) for s in (1, -1)]
    barrier = pltpu.get_barrier_semaphore()
    for axis, step in steps:
        pl.semaphore_signal(
            barrier, inc=1, device_id={axis: place(axis, step)}, device_id_type=MESH
        )

    loads = [
        pltpu.make_async_copy(src, dst, ins.at[n])
        for n, (src, dst) in enumerate(
            (
                (pair_far, pair),
                (w_bias_far, w_bias),
                (mask_far, mask),
                (w_qkvg_far, w_qkvg),
                (cot_far, cot),
                (w_out_far, w_out),
            )
        )
    ]
    for load in loads:
        load.start()
    for load in loads[:2]:
        load.wait()
    standard, inverse = standardized(pair[...].reshape(full_rows * block, channels))
    normed_own = standard.astype(BF16)
    w_rows = w_bias[...].astype(F32)
    flat = over(w_bias[...], normed_own)
    lines = []
    for j in range(full_rows):
        part = flat[:, j * block : (j + 1) * block]
        lines += [jnp.concatenate([part[0:1], part[1:2]], 1)]
    piece[0, lax.axis_index("chan")] = jnp.concatenate(lines, 0)
    for load in loads[2:]:
        load.wait()
    valid = MASK_BIG * (mask[...].astype(F32) - 1.0)
    mask_own[...] = jnp.concatenate([valid, valid], 1)
    wqk = jnp.concatenate([w_qkvg[0], w_qkvg[1]], 0)
    wvg = jnp.concatenate([w_qkvg[2], w_qkvg[3]], 0)
    pl.semaphore_wait(barrier, len(steps))

    head_lane = lax.broadcasted_iota(jnp.int32, (block, cols), 1) < size
    lane = lax.broadcasted_iota(jnp.int32, (tokens, span), 1) < block
    lane_col = lax.broadcasted_iota(jnp.int32, (tokens, cols), 1) < size

    def doubled(values):
        parts = []
        for n in range(width):
            part = values[n * block : (n + 1) * block]
            zero = jnp.zeros_like(part)
            parts += [jnp.where(head_lane, part, zero), jnp.where(head_lane, zero, part)]
        return jnp.concatenate(parts, 0)

    def halved(values):
        parts = []
        for n in range(width):
            first = values[n * span : n * span + block]
            second = values[n * span + block : (n + 1) * span]
            parts += [jnp.where(head_lane, first, second)]
        return jnp.concatenate(parts, 0)

    def per_head(parts, joined, reduced, empty):
        both = functools.reduce(joined, parts)
        first = reduced(jnp.where(lane, both, empty), axis=1, keepdims=True)
        second = reduced(jnp.where(lane, empty, both), axis=1, keepdims=True)
        return jnp.where(lane, first, second)

    core = lax.axis_index("chan")
    halves = ((pair, rows), (cot, cots))
    known = []

    def start_exchange():
        for n, (src, dst) in enumerate(halves):
            for d in (2, 1, 3):
                half = src.at[place("col", d), core]
                remote(half, dst.at[x, core], rs.at[n, d], rr.at[n, d], "col", d).start()
        for d in (2, 1, 3):
            remote(mask_own, masks.at[x], es.at[2], er.at[2, d], "col", d).start()
        rows[x], cots[x], masks[x] = pair[x], cot[x], mask_own[...]

    def hand_over():
        for n, (src, dst) in enumerate(halves):
            for d in range(1, width):
                half = dst.at[place("col", -d), core]
                arrived(half, rr.at[n, d])
                remote(half, half, hs.at[n, d], hr.at[n, d], "chan", 1).start()
        for n, (src, dst) in enumerate(halves):
            for d in range(1, width):
                arrived(src.at[0, 0], rs.at[n, d])

    def project(r):
        normed = standardized(rows[:, r].reshape(tokens, channels))[0].astype(BF16)
        row_cot = cots[:, r].reshape(tokens, channels)
        qk, vg = over(normed, wqk), over(normed, wvg)
        query = (qk[:, :cols] * scale).astype(BF16)
        key2 = doubled(qk[:, cols:]).astype(BF16)
        value2 = doubled(vg[:, :cols]).astype(BF16)
        gate = jax.nn.sigmoid(vg[:, cols:])
        d_gated = over(row_cot, w_out[...])
        d_attended = (d_gated * gate).astype(BF16)
        scores = over(query, key2)
        d_weights = over(d_attended, value2)
        known.append(
            (normed, row_cot, query, key2, value2, gate, d_gated, d_attended, scores, d_weights)
        )

    def first_row():
        for n, (_, dst) in enumerate(halves):
            for d in range(1, width):
                arrived(dst.at[place("col", -d), 1 - core], hr.at[n, d])
                arrived(dst.at[0, 0], hs.at[n, d])
        exchanged(masks, es.at[2], er.at[2])
        project(0)

    def other_rows():
        for r in range(1, row_count):
            project(r)

    gaps = (start_exchange, hand_over, first_row, other_rows)
    gather_everywhere(piece, bias, gzs, gzr, gxs, gxr, gs, gr, gaps)
    blocks = [lax.rem(z + length - b, length) for b in range(length)]

    bias_sum = [None] * width
    saved = []
    for r in range(row_count):
        _, _, _, _, value2, _, _, d_attended, scores, d_weights = known[r]
        parts = [
            (scores[:, n * span : (n + 1) * span] + jnp.concatenate([bias[n, k, core] for k in blocks], 0))
            + masks[n, pl.ds(x * row_count + r, 1), :]
            for n in range(width)
        ]
        top = per_head(parts, jnp.maximum, jnp.max, -jnp.inf)
        parts = [jnp.exp(part - top) for part in parts]
        below = 1.0 / per_head(parts, jnp.add, jnp.sum, 0.0)
        weights = [part * below for part in parts]
        weights_b = jnp.concatenate([w.astype(BF16) for w in weights], 1)
        attended = plain(weights_b, value2)
        product = d_attended.astype(F32) * attended
        first = jnp.sum(jnp.where(lane_col, product, 0.0), axis=1, keepdims=True)
        second = jnp.sum(jnp.where(lane_col, 0.0, product), axis=1, keepdims=True)
        row_dot = jnp.where(lane, first, second)
        d_scores = [
            weights[n] * (d_weights[:, n * span : (n + 1) * span] - row_dot)
            for n in range(width)
        ]
        bias_sum = [d if b is None else b + d for b, d in zip(bias_sum, d_scores)]
        d_scores_b = jnp.concatenate([d.astype(BF16) for d in d_scores], 1)
        saved += [(weights_b, attended, d_scores_b)]
    for n in range(width):
        for b in range(length):
            part = bias_sum[n][b * full_rows : (b + 1) * full_rows]
            d_bias[n, lax.rem(b + length - z, length)] = part.astype(BF16)
    quarter, half = length // 4, length // 2
    step = quarter // 2
    groups = [((half - step, quarter),)]
    groups += [((half - n * step, step), (half + (n - 1) * step, step)) for n in range(2, 5)]

    def send_group(n):
        for first, count in groups[n]:
            slots = pl.ds(first, count)
            for d in (2, 1, 3):
                src = d_bias.at[place("col", d), slots]
                remote(src, bias_in.at[x, slots], bs, br.at[n, d], "col", d).start()

    send_group(0)
    bias_in[x] = d_bias[x]

    gqk = gvg = gout = None
    for r in range(row_count):
        normed, row_cot, query, key2, _, gate, d_gated, d_attended, _, _ = known[r]
        weights_b, attended, d_scores_b = saved[r]
        gated = (gate * attended).astype(BF16)
        upd[:, r] = plain(gated, w_out[...]).astype(BF16).reshape(width, block, channels)
        d_gate = d_gated * attended * gate * (1.0 - gate)
        d_query = plain(d_scores_b, key2) * scale
        d_key = halved(under(d_scores_b, query))
        d_value = halved(under(weights_b, d_attended))
        dqk = jnp.concatenate([d_query, d_key], 1).astype(BF16)
        dvg = jnp.concatenate([d_value, d_gate], 1).astype(BF16)
        back = plain(dqk, wqk) + plain(dvg, wvg)
        dn[:, r] = back.astype(BF16).reshape(width, block, channels)
        new = (under(dqk, normed), under(dvg, normed), under(gated, row_cot))
        if gqk is None:
            gqk, gvg, gout = new
        else:
            gqk, gvg, gout = gqk + new[0], gvg + new[1], gout + new[2]
    part_rows = grads.shape[1]
    everything = jnp.concatenate([gqk, gvg, gout], 0).astype(BF16)
    for n in range(width):
        grads[n] = everything[n * part_rows : (n + 1) * part_rows]
    sources = ((grads, grads_in), (upd, upd_in), (dn, dn_in))
    exchange(grads, grads_in, es.at[3], er.at[3])
    for n in range(1, 4):
        send_group(n)
    exchange(dn, dn_in, es.at[5], er.at[5])
    exchange(upd, upd_in, es.at[4], er.at[4])
    for src, dst in sources:
        dst[x] = src[x]

    def send_tiles(n):
        for d in range(1, width):
            arrived(bias_in.at[0, pl.ds(0, quarter)], br.at[n, d])
        slots = []
        for first, count in groups[n]:
            parts = [bias_in[m, first : first + count].astype(F32) for m in range(width)]
            pieces[first : first + count] = add_up(parts).astype(BF16)
            slots += range(first, first + count)
        for k in sorted(slots, key=lambda k: -min(k, length - k)):
            if k:
                remote(pieces.at[k], tiles.at[k], ls, lr, "row", k).start()

    send_tiles(0)
    exchanged(grads_in, es.at[3], er.at[3])
    summed = add_up([grads_in[n].astype(F32) for n in range(width)]).reshape(-1, HOP, channels)
    shares[...] = summed.astype(BF16)
    used = shares.shape[0]
    for step in reversed(by_distance(length)):
        dest = place("row", step)

        @pl.when(dest < used)
        def _():
            src = shares.at[dest]
            remote(src, shares_in.at[step % length], ss, sr, "row", step).start()

    for n in range(1, 4):
        send_tiles(n)
    tiles[0] = pieces[0]
    exchanged(dn_in, es.at[5], er.at[5])
    exchanged(upd_in, es.at[4], er.at[4])
    other = remote(upd_in, upd_other, cs.at[0], cr.at[0], "chan", 1)
    other.start()
    other.wait()
    update[...] = (upd_in[...].astype(F32) + upd_other[...].astype(F32)).astype(BF16)
    arrived(tiles.at[pl.ds(0, length - 1)], lr)
    tile = jnp.sum(tiles[...].astype(F32), 0)
    columns = jnp.transpose(tile)
    sums = [None, None]
    for j in range(full_rows):
        normed = normed_own[j * block : (j + 1) * block].astype(F32)
        for h in range(2):
            term = normed * columns[h * block : (h + 1) * block, j : j + 1]
            sums[h] = term if sums[h] is None else sums[h] + term
    sums = [jnp.sum(term, 0, keepdims=True) for term in sums]
    bias_own[...] = jnp.concatenate(sums, 0)
    for d in (2, 1, 3):
        remote(bias_own, bias_x.at[x], ws, wr.at[d], "col", d).start()
    bias_x[x] = bias_own[...]
    for j in range(full_rows):
        added = dn_in[j // row_count, j % row_count].astype(F32)
        for h in range(2):
            column = columns[h * block : (h + 1) * block, j : j + 1]
            added = added + column * w_rows[h : h + 1, :]
        dn_mine[j // row_count, j % row_count] = added.astype(BF16)
    other = remote(dn_mine, dn_other, cs.at[1], cr.at[1], "chan", 1)
    other.start()

    @pl.when(z < used)
    def _():
        shares_in[0] = shares[z]
        arrived(shares_in.at[pl.ds(0, length - 1)], sr)
        share_own[...] = jnp.sum(shares_in[...].astype(F32), 0).astype(BF16)
        slot = share_all.at[x, z]
        for step in reversed(by_distance(length)):
            remote(share_own, slot, fs, fr.at[step % length], "row", step).start()
        for d in (2, 1, 3):
            remote(share_own, slot, fxs, fxr.at[d], "col", d).start()
        share_all[x, z] = share_own[...]

    exchanged(bias_x, ws, wr)
    bias_row[...] = jnp.sum(bias_x[...], 0)
    to_all_rows(
        lambda step: bias_row, lambda step: bias_all.at[step % length], vs, lambda step: vr
    )
    bias_all[0] = bias_row[...]

    other.wait()
    d_total = dn_mine[...].astype(F32) + dn_other[...].astype(F32)
    d_total = d_total.reshape(full_rows * block, channels)
    centred = d_total - jnp.mean(d_total, -1, keepdims=True)
    centred = centred - standard * jnp.mean(d_total * standard, -1, keepdims=True)
    grad[...] = (inverse * centred).astype(BF16).reshape(grad.shape)

    for step in by_distance(length):
        source = place("row", -step)

        @pl.when(source < used)
        def _():
            slot = share_all.at[x, source]
            arrived(slot, fr.at[step % length])
            for d in (2, 1, 3):
                remote(slot, slot, fxs, fxr.at[d], "col", d).start()

    arrived(bias_all.at[pl.ds(0, length - 1)], vr)
    for d in range(1, width):
        arrived(share_all.at[place("col", -d)], fxr.at[d])
    arrived(bias_all.at[pl.ds(0, length - 1)], vs)

    @pl.when(z < used)
    def _():
        arrived(shares_in.at[pl.ds(0, length - 1)], fs)
        arrived(shares.at[pl.ds(0, used - 1)], ss)

    @pl.when(z >= used)
    def _():
        arrived(shares, ss)

    arrived(share_all.at[pl.ds(0, width - 1)], fxs)
    arrived(bias_in.at[pl.ds(0, width - 1)], bs)
    arrived(pieces.at[pl.ds(0, length - 1)], ls)


def finish_kernel(tokens, update_in, grad_in, share_all, bias_all, update, grad, qkvg, bias, out):
    update[...] = update_in[...]
    grad[...] = grad_in[...]
    _, cols, channels = qkvg.shape
    total = 4 * cols + out.shape[0]
    rows = share_all[...].astype(F32).reshape(total, channels) / tokens
    qkvg[...] = rows[: 4 * cols].reshape(qkvg.shape)
    out[...] = rows[4 * cols :]
    bias[...] = jnp.sum(bias_all[...], 0) / tokens


def call(kernel, name, identity, outs, scratch, *args, near=pltpu.VMEM):
    params = dict(vmem_limit_bytes=24 * 2**20)
    if identity is not None:
        params.update(collective_id=identity, has_side_effects=True)
    vmem = pl.BlockSpec(memory_space=pltpu.VMEM)
    return pl.pallas_call(
        kernel,
        out_shape=[jax.ShapeDtypeStruct(shape, kind) for shape, kind in outs],
        in_specs=[pl.BlockSpec(memory_space=near)] * len(args),
        out_specs=[vmem] * len(outs),
        scratch_shapes=scratch,
        compiler_params=pltpu.CompilerParams(**params),
        name=name,
    )(*args)


def on_device(pair_rep, pair_mask, w_qkvg, w_bias, w_out, cotangent):
    full_rows, block, channels = pair_rep.shape
    length, width = lax.axis_size("row"), lax.axis_size("col")
    cols = w_qkvg.shape[2]
    heads = w_bias.shape[1]
    scale = (cols // heads) ** (-0.5)
    tokens = width * block
    span = heads * block
    tiled = (width, full_rows // width, block, channels)
    part = (2 * channels + cols) // width
    message = (full_rows, span)
    V = pltpu.VMEM
    gathered = (width, length) + message
    share = (HOP, channels)
    tile = V(tiled, BF16)
    stored = jnp.transpose(w_qkvg, (0, 2, 1))
    args = (
        pair_rep.reshape(tiled),
        cotangent.reshape(tiled),
        pair_mask,
        stored,
        w_bias.T,
        w_out,
    )
    scratch = [V(arg.shape, arg.dtype) for arg in args]
    both = (lax.axis_size("chan"),) + message
    scratch += [V((1,) + both, F32), V((width, length) + both, F32), tile, tile]
    scratch += [V(message, F32), V((width,) + message, F32)]
    scratch += [V(gathered, BF16)] * 2 + [tile] * 7
    scratch += [V((width, part, channels), BF16)] * 2 + [V((length,) + message, BF16)] * 2
    scratch += [V((part // HOP,) + share, BF16), V((length,) + share, BF16), V(share, BF16)]
    scratch += [V((heads, channels), F32), V((width, heads, channels), F32)]
    scratch += [V((heads, channels), F32)]
    scratch += [DMA((len(args),)), DMA, DMA((length,)), DMA, DMA((width,))]
    scratch += [DMA((6,)), DMA((6, width))] + [DMA((2, width))] * 4
    scratch += [DMA((1 + width,)), DMA((1 + width,)), DMA, DMA((4, width))]
    scratch += [DMA, DMA, DMA((2,)), DMA((2,))]
    scratch += [DMA, DMA, DMA, DMA((length,)), DMA, DMA((width,))]
    scratch += [DMA, DMA((width,)), DMA, DMA]
    update, grad, share_all, bias_all = call(
        functools.partial(whole_kernel, scale),
        "whole",
        0,
        [
            (tiled, BF16),
            (tiled, BF16),
            ((width, part // HOP) + share, BF16),
            ((length, heads, channels), F32),
        ],
        scratch,
        *(pltpu.with_memory_space_constraint(arg, pltpu.HBM) for arg in args),
        near=pltpu.HBM,
    )
    shape = pair_rep.shape
    update, grad, qkvg, bias_grad, out = call(
        functools.partial(finish_kernel, tokens),
        "finish",
        None,
        [
            (tiled, BF16),
            (tiled, BF16),
            (stored.shape, F32),
            (w_bias.T.shape, F32),
            (w_out.shape, F32),
        ],
        [],
        update,
        grad,
        share_all,
        bias_all,
    )
    qkvg = jnp.transpose(qkvg, (0, 2, 1))
    return (update.reshape(shape), grad.reshape(shape), qkvg, bias_grad.T, out)


def solution(mesh):
    in_specs = (
        P(("groups", "row"), "col", None),
        P(("groups", "row"), "col"),
        P(None, None, "chan"),
        P(None, "chan"),
        P("chan", None),
        P(("groups", "row"), "col", None),
    )
    out_specs = (
        P(("groups", "row"), "col", None),
        P(("groups", "row"), "col", None),
        P("groups", None, "chan"),
        P("groups", "chan"),
        P("chan", "groups"),
    )
    return jax.shard_map(
        on_device, mesh=mesh, in_specs=in_specs, out_specs=out_specs, check_vma=False
    )
```

```python
import functools

import jax
import jax.numpy as jnp
from jax import lax
from jax.experimental import pallas as pl
from jax.experimental.pallas import tpu as pltpu
from jax.sharding import PartitionSpec as P

EPSILON = 1e-05
MASK_BIG = 1000000000.0
MESH = pl.DeviceIdType.MESH
F32 = jnp.float32
BF16 = jnp.bfloat16
HOP = 4
DMA = pltpu.SemaphoreType.DMA


def place(axis, step):
    size = lax.axis_size(axis)
    return lax.rem(lax.axis_index(axis) + (step % size), size)


def remote(src, dst, send, recv, axis, step):
    return pltpu.make_async_remote_copy(
        src_ref=src,
        dst_ref=dst,
        send_sem=send,
        recv_sem=recv,
        device_id={axis: place(axis, step)},
        device_id_type=MESH,
    )


def arrived(dst, recv):
    pltpu.make_async_copy(dst, dst, recv).wait()


def gather_everywhere(piece, out, zs, zr, xs, xr, gaps):
    length, width = lax.axis_size("row"), lax.axis_size("col")
    x, half = lax.axis_index("col"), length // 2
    last = half // HOP

    def along_row(src, delta, steps):
        for step in steps:
            k = (delta + step) % length
            remote(src, out.at[x, k], zs, zr.at[k], "row", step).start()

    def along_col(src, first, count):
        slots = out.at[x, pl.ds(first, count)]
        for d in (2, 1, 3):
            remote(slots if src is None else src, slots, xs, xr.at[d], "col", d).start()

    def wait(delta):
        arrived(out.at[x, delta % length], zr.at[delta % length])

    along_row(piece.at[0], 0, [s * t for t in (HOP, 3, 2, 1) for s in (1, -1)])
    along_col(piece, 0, 1)
    out[x, 0] = piece[0]
    gaps[0]()
    for a in range(1, last):
        for s in (1, -1):
            wait(s * HOP * a)
            far = [s * HOP] if (s == 1 or a < last - 1) else []
            along_row(out.at[x, s * HOP * a % length], s * HOP * a, far + [s * t for t in (3, 2, 1)])
        for s in (1, -1):
            for t in range(1, HOP):
                wait(s * (HOP * (a - 1) + t))
            along_col(None, HOP * (a - 1) + 1 if s == 1 else length - HOP * a, HOP)
        gaps[a]()
    for t in range(1, HOP):
        for s in (1, -1):
            wait(s * (half - HOP + t))
    along_col(None, half + 1, HOP - 1)
    along_col(None, half - HOP + 1, HOP - 1)
    wait(half)
    along_col(None, half, 1)
    for d in range(1, width):
        arrived(out.at[place("col", -d)], xr.at[d])


def by_distance(length):
    return [s * t for t in range(1, length // 2) for s in (1, -1)] + [length // 2]


def to_all_rows(src_of, dst_of, send, recv_of):
    for step in reversed(by_distance(lax.axis_size("row"))):
        remote(src_of(step), dst_of(step), send, recv_of(step), "row", step).start()


def exchange(src, dst, xs, xr):
    for d in (2, 1, 3):
        remote(
            src.at[place("col", d)], dst.at[lax.axis_index("col")], xs, xr.at[d], "col", d
        ).start()


def exchanged(dst, xs, xr):
    for d in range(1, lax.axis_size("col")):
        arrived(dst.at[place("col", -d)], xr.at[d])
    arrived(dst.at[pl.ds(0, lax.axis_size("col") - 1)], xs)


def over(a, b):
    return lax.dot_general(a, b, (((1,), (1,)), ((), ())), preferred_element_type=F32)


def under(a, b):
    return lax.dot_general(a, b, (((0,), (0,)), ((), ())), preferred_element_type=F32)


def plain(a, b):
    return lax.dot_general(a, b, (((1,), (0,)), ((), ())), preferred_element_type=F32)


def standardized(values):
    values = values.astype(F32)
    centred = values - jnp.mean(values, -1, keepdims=True)
    inverse = lax.rsqrt(jnp.mean(centred * centred, -1, keepdims=True) + EPSILON)
    return centred * inverse, inverse


def add_up(values):
    return functools.reduce(jnp.add, values)


def whole_kernel(
    scale, pair_far, cot_far, mask_far, w_qkvg_far, w_bias_far, w_out_far, update, grad, share_all,
    bias_all, pair, cot, mask, w_qkvg, w_bias, w_out, piece, bias, rows, cots, mask_own, masks,
    d_bias, bias_in, upd, upd_in, upd_other, dn, dn_in, dn_mine, dn_other, grads, grads_in, pieces,
    tiles, shares, shares_in, share_own, bias_own, bias_x, bias_row, ins, gzs, gzr, gxs, gxr, es,
    er, rs, rr, hs, hr, bs, br, ls, lr, cs, cr, ss, sr, fs, fr, fxs, fxr, ws, wr, vs, vr,
):
    length, width = lax.axis_size("row"), lax.axis_size("col")
    x, z = lax.axis_index("col"), lax.axis_index("row")
    _, row_count, block, channels = pair.shape
    cols = w_out.shape[0]
    size = cols // 2
    tokens, span = width * block, 2 * block
    full_rows = width * row_count
    steps = [("chan", 1)] + [("col", d) for d in range(1, width)]
    steps += [("row", s * t) for t in range(1, HOP + 1) for s in (1, -1)]
    barrier = pltpu.get_barrier_semaphore()
    for axis, step in steps:
        pl.semaphore_signal(
            barrier, inc=1, device_id={axis: place(axis, step)}, device_id_type=MESH
        )

    loads = [
        pltpu.make_async_copy(src, dst, ins.at[n])
        for n, (src, dst) in enumerate(
            (
                (pair_far, pair),
                (w_bias_far, w_bias),
                (mask_far, mask),
                (w_qkvg_far, w_qkvg),
                (cot_far, cot),
                (w_out_far, w_out),
            )
        )
    ]
    for load in loads:
        load.start()
    for load in loads[:2]:
        load.wait()
    standard, inverse = standardized(pair[...].reshape(full_rows * block, channels))
    normed_own = standard.astype(BF16)
    w_rows = w_bias[...].astype(F32)
    flat = over(w_bias[...], normed_own)
    lines = []
    for j in range(full_rows):
        part = flat[:, j * block : (j + 1) * block]
        lines += [jnp.concatenate([part[0:1], part[1:2]], 1)]
    piece[0] = jnp.concatenate(lines, 0)
    for load in loads[2:]:
        load.wait()
    valid = MASK_BIG * (mask[...].astype(F32) - 1.0)
    mask_own[...] = jnp.concatenate([valid, valid], 1)
    wqk = jnp.concatenate([w_qkvg[0], w_qkvg[1]], 0)
    wvg = jnp.concatenate([w_qkvg[2], w_qkvg[3]], 0)
    pl.semaphore_wait(barrier, len(steps))

    head_lane = lax.broadcasted_iota(jnp.int32, (block, cols), 1) < size
    lane = lax.broadcasted_iota(jnp.int32, (tokens, span), 1) < block
    lane_col = lax.broadcasted_iota(jnp.int32, (tokens, cols), 1) < size

    def doubled(values):
        parts = []
        for n in range(width):
            part = values[n * block : (n + 1) * block]
            zero = jnp.zeros_like(part)
            parts += [jnp.where(head_lane, part, zero), jnp.where(head_lane, zero, part)]
        return jnp.concatenate(parts, 0)

    def halved(values):
        parts = []
        for n in range(width):
            first = values[n * span : n * span + block]
            second = values[n * span + block : (n + 1) * span]
            parts += [jnp.where(head_lane, first, second)]
        return jnp.concatenate(parts, 0)

    def per_head(parts, joined, reduced, empty):
        both = functools.reduce(joined, parts)
        first = reduced(jnp.where(lane, both, empty), axis=1, keepdims=True)
        second = reduced(jnp.where(lane, empty, both), axis=1, keepdims=True)
        return jnp.where(lane, first, second)

    core = lax.axis_index("chan")
    halves = ((pair, rows), (cot, cots))
    known = []

    def start_exchange():
        for n, (src, dst) in enumerate(halves):
            for d in (2, 1, 3):
                half = src.at[place("col", d), core]
                remote(half, dst.at[x, core], rs.at[n, d], rr.at[n, d], "col", d).start()
        for d in (2, 1, 3):
            remote(mask_own, masks.at[x], es.at[2], er.at[2, d], "col", d).start()
        rows[x], cots[x], masks[x] = pair[x], cot[x], mask_own[...]

    def hand_over():
        for n, (src, dst) in enumerate(halves):
            for d in range(1, width):
                half = dst.at[place("col", -d), core]
                arrived(half, rr.at[n, d])
                remote(half, half, hs.at[n, d], hr.at[n, d], "chan", 1).start()
    def project(r):
        normed = standardized(rows[:, r].reshape(tokens, channels))[0].astype(BF16)
        row_cot = cots[:, r].reshape(tokens, channels)
        qk, vg = over(normed, wqk), over(normed, wvg)
        query = (qk[:, :cols] * scale).astype(BF16)
        key2 = doubled(qk[:, cols:]).astype(BF16)
        value2 = doubled(vg[:, :cols]).astype(BF16)
        gate = jax.nn.sigmoid(vg[:, cols:])
        d_gated = over(row_cot, w_out[...])
        d_attended = (d_gated * gate).astype(BF16)
        scores = over(query, key2)
        d_weights = over(d_attended, value2)
        known.append(
            (normed, row_cot, query, key2, value2, gate, d_gated, d_attended, scores, d_weights)
        )

    def project_all():
        for n, (_, dst) in enumerate(halves):
            for d in range(1, width):
                arrived(dst.at[place("col", -d), 1 - core], hr.at[n, d])
        exchanged(masks, es.at[2], er.at[2])
        for r in range(row_count):
            project(r)

    gaps = (start_exchange, lambda: None, hand_over, project_all)
    gather_everywhere(piece, bias, gzs, gzr, gxs, gxr, gaps)
    blocks = [lax.rem(z + length - b, length) for b in range(length)]

    bias_sum = [None] * width
    saved = []
    for r in range(row_count):
        _, _, _, _, value2, _, _, d_attended, scores, d_weights = known[r]
        parts = [
            (scores[:, n * span : (n + 1) * span] + jnp.concatenate([bias[n, k] for k in blocks], 0))
            + masks[n, pl.ds(x * row_count + r, 1), :]
            for n in range(width)
        ]
        top = per_head(parts, jnp.maximum, jnp.max, -jnp.inf)
        parts = [jnp.exp(part - top) for part in parts]
        below = 1.0 / per_head(parts, jnp.add, jnp.sum, 0.0)
        weights = [part * below for part in parts]
        weights_b = jnp.concatenate([w.astype(BF16) for w in weights], 1)
        attended = plain(weights_b, value2)
        product = d_attended.astype(F32) * attended
        first = jnp.sum(jnp.where(lane_col, product, 0.0), axis=1, keepdims=True)
        second = jnp.sum(jnp.where(lane_col, 0.0, product), axis=1, keepdims=True)
        row_dot = jnp.where(lane, first, second)
        d_scores = [
            weights[n] * (d_weights[:, n * span : (n + 1) * span] - row_dot)
            for n in range(width)
        ]
        bias_sum = [d if b is None else b + d for b, d in zip(bias_sum, d_scores)]
        d_scores_b = jnp.concatenate([d.astype(BF16) for d in d_scores], 1)
        saved += [(weights_b, attended, d_scores_b)]
    for n in range(width):
        for b in range(length):
            part = bias_sum[n][b * full_rows : (b + 1) * full_rows]
            d_bias[n, lax.rem(b + length - z, length)] = part.astype(BF16)
    quarter, half = length // 4, length // 2
    step = quarter // 2
    groups = [((half - step, quarter),)]
    groups += [((half - n * step, step), (half + (n - 1) * step, step)) for n in range(2, 5)]

    def send_group(n):
        for first, count in groups[n]:
            slots = pl.ds(first, count)
            for d in (2, 1, 3):
                src = d_bias.at[place("col", d), slots]
                remote(src, bias_in.at[x, slots], bs, br.at[n, d], "col", d).start()

    send_group(0)
    bias_in[x] = d_bias[x]

    gqk = gvg = gout = None
    for r in range(row_count):
        normed, row_cot, query, key2, _, gate, d_gated, d_attended, _, _ = known[r]
        weights_b, attended, d_scores_b = saved[r]
        gated = (gate * attended).astype(BF16)
        upd[:, r] = plain(gated, w_out[...]).astype(BF16).reshape(width, block, channels)
        d_gate = d_gated * attended * gate * (1.0 - gate)
        d_query = plain(d_scores_b, key2) * scale
        d_key = halved(under(d_scores_b, query))
        d_value = halved(under(weights_b, d_attended))
        dqk = jnp.concatenate([d_query, d_key], 1).astype(BF16)
        dvg = jnp.concatenate([d_value, d_gate], 1).astype(BF16)
        back = plain(dqk, wqk) + plain(dvg, wvg)
        dn[:, r] = back.astype(BF16).reshape(width, block, channels)
        new = (under(dqk, normed), under(dvg, normed), under(gated, row_cot))
        if gqk is None:
            gqk, gvg, gout = new
        else:
            gqk, gvg, gout = gqk + new[0], gvg + new[1], gout + new[2]
    part_rows = grads.shape[1]
    everything = jnp.concatenate([gqk, gvg, gout], 0).astype(BF16)
    for n in range(width):
        grads[n] = everything[n * part_rows : (n + 1) * part_rows]
    sources = ((grads, grads_in), (upd, upd_in), (dn, dn_in))
    exchange(grads, grads_in, es.at[3], er.at[3])
    for n in range(1, 4):
        send_group(n)
    exchange(dn, dn_in, es.at[5], er.at[5])
    exchange(upd, upd_in, es.at[4], er.at[4])
    for src, dst in sources:
        dst[x] = src[x]

    def send_tiles(n):
        for d in range(1, width):
            arrived(bias_in.at[0, pl.ds(0, quarter)], br.at[n, d])
        slots = []
        for first, count in groups[n]:
            parts = [bias_in[m, first : first + count].astype(F32) for m in range(width)]
            pieces[first : first + count] = add_up(parts).astype(BF16)
            slots += range(first, first + count)
        for k in sorted(slots, key=lambda k: -min(k, length - k)):
            if k:
                remote(pieces.at[k], tiles.at[k], ls, lr, "row", k).start()

    send_tiles(0)
    exchanged(grads_in, es.at[3], er.at[3])
    summed = add_up([grads_in[n].astype(F32) for n in range(width)]).reshape(-1, HOP, channels)
    shares[...] = summed.astype(BF16)
    used = shares.shape[0]
    for step in reversed(by_distance(length)):
        dest = place("row", step)

        @pl.when(dest < used)
        def _():
            src = shares.at[dest]
            remote(src, shares_in.at[step % length], ss, sr, "row", step).start()

    for n in range(1, 4):
        send_tiles(n)
    tiles[0] = pieces[0]
    exchanged(dn_in, es.at[5], er.at[5])
    exchanged(upd_in, es.at[4], er.at[4])
    other = remote(upd_in, upd_other, cs.at[0], cr.at[0], "chan", 1)
    other.start()
    other.wait()
    update[...] = (upd_in[...].astype(F32) + upd_other[...].astype(F32)).astype(BF16)
    arrived(tiles.at[pl.ds(0, length - 1)], lr)
    tile = jnp.sum(tiles[...].astype(F32), 0)
    columns = jnp.transpose(tile)
    sums = [None, None]
    for j in range(full_rows):
        normed = normed_own[j * block : (j + 1) * block].astype(F32)
        for h in range(2):
            term = normed * columns[h * block : (h + 1) * block, j : j + 1]
            sums[h] = term if sums[h] is None else sums[h] + term
    sums = [jnp.sum(term, 0, keepdims=True) for term in sums]
    bias_own[...] = jnp.concatenate(sums, 0)
    for d in (2, 1, 3):
        remote(bias_own, bias_x.at[x], ws, wr.at[d], "col", d).start()
    bias_x[x] = bias_own[...]
    for j in range(full_rows):
        added = dn_in[j // row_count, j % row_count].astype(F32)
        for h in range(2):
            column = columns[h * block : (h + 1) * block, j : j + 1]
            added = added + column * w_rows[h : h + 1, :]
        dn_mine[j // row_count, j % row_count] = added.astype(BF16)
    other = remote(dn_mine, dn_other, cs.at[1], cr.at[1], "chan", 1)
    other.start()

    @pl.when(z < used)
    def _():
        shares_in[0] = shares[z]
        arrived(shares_in.at[pl.ds(0, length - 1)], sr)
        share_own[...] = jnp.sum(shares_in[...].astype(F32), 0).astype(BF16)
        slot = share_all.at[x, z]
        for step in reversed(by_distance(length)):
            remote(share_own, slot, fs, fr.at[step % length], "row", step).start()
        for d in (2, 1, 3):
            remote(share_own, slot, fxs, fxr.at[d], "col", d).start()
        share_all[x, z] = share_own[...]

    exchanged(bias_x, ws, wr)
    bias_row[...] = jnp.sum(bias_x[...], 0)
    to_all_rows(
        lambda step: bias_row, lambda step: bias_all.at[step % length], vs, lambda step: vr
    )
    bias_all[0] = bias_row[...]

    other.wait()
    d_total = dn_mine[...].astype(F32) + dn_other[...].astype(F32)
    d_total = d_total.reshape(full_rows * block, channels)
    centred = d_total - jnp.mean(d_total, -1, keepdims=True)
    centred = centred - standard * jnp.mean(d_total * standard, -1, keepdims=True)
    grad[...] = (inverse * centred).astype(BF16).reshape(grad.shape)

    for step in by_distance(length):
        source = place("row", -step)

        @pl.when(source < used)
        def _():
            slot = share_all.at[x, source]
            arrived(slot, fr.at[step % length])
            for d in (2, 1, 3):
                remote(slot, slot, fxs, fxr.at[d], "col", d).start()

    arrived(bias_all.at[pl.ds(0, length - 1)], vr)
    for d in range(1, width):
        arrived(share_all.at[place("col", -d)], fxr.at[d])
    arrived(bias_all.at[pl.ds(0, length - 1)], vs)

    @pl.when(z < used)
    def _():
        arrived(shares_in.at[pl.ds(0, length - 1)], fs)
        arrived(shares.at[pl.ds(0, used - 1)], ss)

    @pl.when(z >= used)
    def _():
        arrived(shares, ss)

    arrived(share_all.at[pl.ds(0, width - 1)], fxs)
    arrived(bias.at[0, pl.ds(0, length - 1)], gzs)
    arrived(bias.at[pl.ds(0, width - 1)], gxs)
    arrived(bias_in.at[pl.ds(0, width - 1)], bs)
    arrived(pieces.at[pl.ds(0, length - 1)], ls)
    for n, (src, dst) in enumerate(halves):
        for d in range(1, width):
            arrived(src.at[0, 0], rs.at[n, d])
            arrived(dst.at[0, 0], hs.at[n, d])


def finish_kernel(tokens, update_in, grad_in, share_all, bias_all, update, grad, qkvg, bias, out):
    update[...] = update_in[...]
    grad[...] = grad_in[...]
    _, cols, channels = qkvg.shape
    total = 4 * cols + out.shape[0]
    rows = share_all[...].astype(F32).reshape(total, channels) / tokens
    qkvg[...] = rows[: 4 * cols].reshape(qkvg.shape)
    out[...] = rows[4 * cols :]
    bias[...] = jnp.sum(bias_all[...], 0) / tokens


def call(kernel, name, identity, outs, scratch, *args, near=pltpu.VMEM):
    params = dict(vmem_limit_bytes=24 * 2**20)
    if identity is not None:
        params.update(collective_id=identity, has_side_effects=True)
    vmem = pl.BlockSpec(memory_space=pltpu.VMEM)
    return pl.pallas_call(
        kernel,
        out_shape=[jax.ShapeDtypeStruct(shape, kind) for shape, kind in outs],
        in_specs=[pl.BlockSpec(memory_space=near)] * len(args),
        out_specs=[vmem] * len(outs),
        scratch_shapes=scratch,
        compiler_params=pltpu.CompilerParams(**params),
        name=name,
    )(*args)


def on_device(pair_rep, pair_mask, w_qkvg, w_bias, w_out, cotangent):
    full_rows, block, channels = pair_rep.shape
    length, width = lax.axis_size("row"), lax.axis_size("col")
    cols = w_qkvg.shape[2]
    heads = w_bias.shape[1]
    scale = (cols // heads) ** (-0.5)
    tokens = width * block
    span = heads * block
    tiled = (width, full_rows // width, block, channels)
    part = (2 * channels + cols) // width
    message = (full_rows, span)
    V = pltpu.VMEM
    gathered = (width, length) + message
    share = (HOP, channels)
    tile = V(tiled, BF16)
    stored = jnp.transpose(w_qkvg, (0, 2, 1))
    args = (
        pair_rep.reshape(tiled),
        cotangent.reshape(tiled),
        pair_mask,
        stored,
        w_bias.T,
        w_out,
    )
    scratch = [V(arg.shape, arg.dtype) for arg in args]
    scratch += [V((1,) + message, F32), V(gathered, F32), tile, tile]
    scratch += [V(message, F32), V((width,) + message, F32)]
    scratch += [V(gathered, BF16)] * 2 + [tile] * 7
    scratch += [V((width, part, channels), BF16)] * 2 + [V((length,) + message, BF16)] * 2
    scratch += [V((part // HOP,) + share, BF16), V((length,) + share, BF16), V(share, BF16)]
    scratch += [V((heads, channels), F32), V((width, heads, channels), F32)]
    scratch += [V((heads, channels), F32)]
    scratch += [DMA((len(args),)), DMA, DMA((length,)), DMA, DMA((width,))]
    scratch += [DMA((6,)), DMA((6, width))] + [DMA((2, width))] * 4 + [DMA, DMA((4, width))]
    scratch += [DMA, DMA, DMA((2,)), DMA((2,))]
    scratch += [DMA, DMA, DMA, DMA((length,)), DMA, DMA((width,))]
    scratch += [DMA, DMA((width,)), DMA, DMA]
    update, grad, share_all, bias_all = call(
        functools.partial(whole_kernel, scale),
        "whole",
        0,
        [
            (tiled, BF16),
            (tiled, BF16),
            ((width, part // HOP) + share, BF16),
            ((length, heads, channels), F32),
        ],
        scratch,
        *(pltpu.with_memory_space_constraint(arg, pltpu.HBM) for arg in args),
        near=pltpu.HBM,
    )
    shape = pair_rep.shape
    update, grad, qkvg, bias_grad, out = call(
        functools.partial(finish_kernel, tokens),
        "finish",
        None,
        [
            (tiled, BF16),
            (tiled, BF16),
            (stored.shape, F32),
            (w_bias.T.shape, F32),
            (w_out.shape, F32),
        ],
        [],
        update,
        grad,
        share_all,
        bias_all,
    )
    qkvg = jnp.transpose(qkvg, (0, 2, 1))
    return (update.reshape(shape), grad.reshape(shape), qkvg, bias_grad.T, out)


def solution(mesh):
    in_specs = (
        P(("groups", "row"), "col", None),
        P(("groups", "row"), "col"),
        P(None, None, "chan"),
        P(None, "chan"),
        P("chan", None),
        P(("groups", "row"), "col", None),
    )
    out_specs = (
        P(("groups", "row"), "col", None),
        P(("groups", "row"), "col", None),
        P("groups", None, "chan"),
        P("groups", "chan"),
        P("chan", "groups"),
    )
    return jax.shard_map(
        on_device, mesh=mesh, in_specs=in_specs, out_specs=out_specs, check_vma=False
    )
```
